256 devices in a mesh: first: 16 (over z, core), second: 16 (over y, x).
Axes of the slice: x: 4, y: 4, z: 8, core: 2. Of those that a mesh axis runs over, the one named last changes fastest.
Arguments:
- pair_rows: bfloat16 [768, 768, 128], P('first', 'second'), may hold values from -6 to 6
- in_gain: float32 [128], replicated, may hold values from 0.25 to 1.75
- left_weight: bfloat16 [128, 128], replicated, may hold values from -0.5 to 0.5
- right_weight: bfloat16 [128, 128], replicated, may hold values from -0.5 to 0.5
- mid_gain: float32 [128], replicated, may hold values from 0.25 to 1.75
- out_weight: bfloat16 [128, 128], replicated, may hold values from -0.5 to 0.5
- out_gate: bfloat16 [128, 128], replicated, may hold values from -0.5 to 0.5
Outputs:
- triangle_out: bfloat16 [768, 768, 128], P('first', 'second')
The draws below stay inside these ranges and needn't reach their ends.
All inputs are finite; a program needn't handle non-finite values.
Results may differ from the reference program's by a relative error of at most 0.012.
Values may be sent and summed in bfloat16 or wider, within the bound.
A program may use at most 64 MiB of HBM per device.

```python
import jax
import jax.numpy as jnp
from jax import lax

RESIDUES = 768
PAIR_WIDTH = 128
MIX_WIDTH = 128


def steps_of(stream_key, dims, cuts, smallest, top_value):
    def one(position, shards_of):
        draws = jax.random.uniform(jax.random.fold_in(jax.random.fold_in(stream_key, 6), position), (shards_of,), jnp.float32, smallest / len(cuts), top_value / len(cuts))
        return jnp.repeat(jnp.exp(draws), dims[position] // shards_of).reshape((-1,) + (1,) * (len(dims) - position - 1))

    level = one(*cuts[0])
    for cut in cuts[1:]:
        level = level * one(*cut)
    return level


def gaussian(stream_key, dims, spread, limit, cuts=(), held_as=jnp.bfloat16):
    values = spread * jax.random.normal(stream_key, dims, jnp.float32)
    if cuts:
        values = values * steps_of(stream_key, dims, cuts, -0.22, 0.18)
    return jnp.clip(values, -limit, limit).astype(held_as)


def setup_inputs(seed: int = 0) -> dict:
    key_list = jax.random.split(jax.random.key(seed), 8)
    pair_rows = gaussian(key_list[0], (RESIDUES, RESIDUES, PAIR_WIDTH), 1.0, 6.0, ((0, 16), (1, 16)))
    in_gain = jnp.clip(1.0 + 0.15 * jax.random.normal(key_list[1], (PAIR_WIDTH,), jnp.float32), 0.25, 1.75)
    left_weight = gaussian(key_list[2], (PAIR_WIDTH, MIX_WIDTH), PAIR_WIDTH ** -0.5, 0.5)
    right_weight = gaussian(key_list[3], (PAIR_WIDTH, MIX_WIDTH), PAIR_WIDTH ** -0.5, 0.5)
    mid_gain = jnp.clip(1.0 + 0.15 * jax.random.normal(key_list[4], (MIX_WIDTH,), jnp.float32), 0.25, 1.75)
    out_weight = gaussian(key_list[5], (MIX_WIDTH, PAIR_WIDTH), MIX_WIDTH ** -0.5, 0.5)
    out_gate = gaussian(key_list[6], (PAIR_WIDTH, PAIR_WIDTH), PAIR_WIDTH ** -0.5, 0.5)
    return {"pair_rows": pair_rows, "in_gain": in_gain, "left_weight": left_weight, "right_weight": right_weight, "mid_gain": mid_gain, "out_weight": out_weight, "out_gate": out_gate}


def norm_channels(values, channel_gain):
    centred = values - lax.optimization_barrier(jnp.mean(values, axis=-1, keepdims=True))
    return centred * lax.rsqrt(lax.optimization_barrier(jnp.mean(centred * centred, axis=-1, keepdims=True)) + 1e-05) * channel_gain

def project_pair(pair_in, in_gain, left_weight, right_weight):
    ready = norm_channels(pair_in.astype(jnp.float32), in_gain).astype(jnp.bfloat16)
    ready = lax.optimization_barrier(ready)
    left = jnp.einsum('ijc,cd->ijd', ready.astype(jnp.float32), left_weight.astype(jnp.float32))
    right = jnp.einsum('ijc,cd->ijd', ready.astype(jnp.float32), right_weight.astype(jnp.float32))
    return (ready, left.astype(jnp.bfloat16), right.astype(jnp.bfloat16))

def to_pair(mixed, ready, mid_gain, out_weight, out_gate):
    scaled = norm_channels(mixed.astype(jnp.float32), mid_gain).astype(jnp.bfloat16)
    scaled = lax.optimization_barrier(scaled)
    gate = jax.nn.sigmoid(jnp.einsum('ijc,cd->ijd', ready.astype(jnp.float32), out_gate.astype(jnp.float32)))
    return (jnp.einsum('ijd,dc->ijc', scaled.astype(jnp.float32), out_weight.astype(jnp.float32)) * gate).astype(jnp.bfloat16)

def reference(pair_rows, in_gain, left_weight, right_weight, mid_gain, out_weight, out_gate):
    ready, left, right = project_pair(pair_rows, in_gain, left_weight, right_weight)
    left, right = lax.optimization_barrier((left, right))

    def one_channel(pair_of):
        return (jnp.dot(pair_of[0].T, pair_of[1], preferred_element_type=jnp.float32) * RESIDUES ** (-0.5)).astype(jnp.bfloat16)
    mixed = jnp.moveaxis(lax.map(one_channel, (jnp.moveaxis(left, -1, 0), jnp.moveaxis(right, -1, 0))), 0, -1)
    mixed = lax.optimization_barrier(mixed)
    return to_pair(mixed, ready, mid_gain, out_weight, out_gate)
```

```python
import functools

import jax
import jax.numpy as jnp
from jax import lax
from jax.experimental import pallas as pl
from jax.experimental.pallas import tpu as pltpu
from jax.sharding import PartitionSpec as P

MESH = pl.DeviceIdType.MESH


def norm_channels(values, channel_gain):
    centred = values - jnp.mean(values, axis=-1, keepdims=True)
    return (
        centred
        * lax.rsqrt(jnp.mean(centred * centred, axis=-1, keepdims=True) + 1e-05)
        * channel_gain
    )


def exchange_kernel(rows, x_ref, o_ref, send_sem, recv_sem, own_sem):
    first, second = lax.axis_index("first"), lax.axis_index("second")
    z, core, y, x = first // 2, first % 2, second // 4, second % 4
    me = z * 16 + second

    def peer(step):
        dz, dy, dx = step // 16, (step // 4) % 4, step % 4
        pz, ps = (z + dz) % 8, ((y + dy) % 4) * 4 + (x + dx) % 4
        return pz * 16 + ps, (pz * 2 + core, ps)

    barrier = pltpu.get_barrier_semaphore()

    def greet(step, _):
        pl.semaphore_signal(barrier, inc=1, device_id=peer(step)[1], device_id_type=MESH)
        return 0

    lax.fori_loop(1, 128, greet, 0)
    pl.semaphore_wait(barrier, 127)

    def send(step, _):
        chip, device = peer(step)
        pltpu.make_async_remote_copy(
            src_ref=x_ref.at[chip],
            dst_ref=o_ref.at[me],
            send_sem=send_sem,
            recv_sem=recv_sem,
            device_id=device,
            device_id_type=MESH,
        ).start()
        return 0

    lax.fori_loop(1, 128, send, 0)
    o_ref[me] = x_ref[me]
    pltpu.make_async_copy(x_ref.at[pl.ds(0, 127)], o_ref.at[pl.ds(0, 127)], recv_sem).wait()
    pltpu.make_async_copy(x_ref.at[pl.ds(0, 127)], o_ref.at[pl.ds(0, 127)], send_sem).wait()


def exchange(x, number):
    return pl.pallas_call(
        functools.partial(exchange_kernel, x.shape[1]),
        out_shape=jax.ShapeDtypeStruct(x.shape, x.dtype),
        in_specs=[pl.BlockSpec(memory_space=pltpu.VMEM)],
        out_specs=pl.BlockSpec(memory_space=pltpu.VMEM),
        scratch_shapes=[pltpu.SemaphoreType.DMA, pltpu.SemaphoreType.DMA, pltpu.SemaphoreType.DMA],
        compiler_params=pltpu.CompilerParams(collective_id=number, has_side_effects=True),
    )(x)


def shards(pair_rows, in_gain, left_weight, right_weight, mid_gain, out_weight, out_gate):
    ready = norm_channels(pair_rows.astype(jnp.float32), in_gain).astype(jnp.bfloat16)
    ready = lax.optimization_barrier(ready)
    both = jnp.concatenate([left_weight, right_weight], axis=1)
    lr = jnp.einsum("kic,cd->dki", ready, both, preferred_element_type=jnp.float32)
    lr = lr.astype(jnp.bfloat16).reshape(2, 128, 18, 128).transpose(1, 0, 2, 3).reshape(128, 36, 128)
    got = exchange(lr, 0).reshape(8, 16, 2, 48, 48)
    got = got.transpose(2, 0, 3, 1, 4).reshape(2, 384, 768)
    part = jnp.einsum("ki,kj->ij", got[0], got[1], preferred_element_type=jnp.float32)
    core = lax.axis_index("first") % 2
    part = part.reshape(8, 2, 48, 768)
    mine = jnp.where(core == 0, part[:, 0], part[:, 1])
    other = jnp.where(core == 0, part[:, 1], part[:, 0])
    swap = [(i, i ^ 1) for i in range(16)]
    mixed = (mine + lax.ppermute(other, "first", swap)) * 768 ** (-0.5)
    mixed = mixed.astype(jnp.bfloat16).reshape(8, 48, 16, 48).transpose(0, 2, 1, 3).reshape(128, 18, 128)
    mixed = exchange(mixed, 1).reshape(128, 48, 48).transpose(1, 2, 0)
    scaled = norm_channels(mixed.astype(jnp.float32), mid_gain).astype(jnp.bfloat16)
    scaled = lax.optimization_barrier(scaled)
    gate = jax.nn.sigmoid(jnp.einsum("ijc,cd->ijd", ready, out_gate, preferred_element_type=jnp.float32))
    return (
        jnp.einsum("ijd,dc->ijc", scaled, out_weight, preferred_element_type=jnp.float32) * gate
    ).astype(jnp.bfloat16)


def solution(mesh):
    in_specs = (P("first", "second", None), P(), P(), P(), P(), P(), P())
    out_specs = P("first", "second", None)
    return jax.shard_map(shards, mesh=mesh, in_specs=in_specs, out_specs=out_specs, check_vma=False)
```

```python
import jax
import jax.numpy as jnp
from jax import lax
from jax.experimental import pallas as pl
from jax.experimental.pallas import tpu as pltpu
from jax.sharding import PartitionSpec as P

MESH = pl.DeviceIdType.MESH
F32, BF16 = jnp.float32, jnp.bfloat16
PITCH = 104
HALF = 56


def swap_blocks(parts):
    block = lax.broadcasted_iota(jnp.int32, parts[0].shape, 1) // 16
    for h in (4, 2, 1):
        low = (block // h) % 2 == 0
        out = list(parts)
        for p in range(8):
            if p // h % 2 == 0:
                a, b = parts[p], parts[p + h]
                out[p] = jnp.where(low, a, pltpu.roll(b, 16 * h, 1))
                out[p + h] = jnp.where(low, pltpu.roll(a, 128 - 16 * h, 1), b)
        parts = out
    return parts


def kernel(
    x_ref, in_gain, left_w, right_w, mid_gain, out_w, gate_w, o_ref,
    weights, ready, wide, sent, got, spread, left, right, sums, other, wide2, sent2, got2, spread2, gates, gain_col,
    send_a, recv_a, send_b, recv_b, send_c, recv_c,
):
    first, second = lax.axis_index("first"), lax.axis_index("second")
    z, core, y, x = first // 2, first % 2, second // 4, second % 4
    me = second * 8 + z
    partner = (z * 2 + 1 - core, second)

    def peer(step):
        dz, dy, dx = step // 16, (step // 4) % 4, step % 4
        pz, ps = (z + dz) % 8, ((y + dy) % 4) * 4 + (x + dx) % 4
        return ps * 8 + pz, (pz * 2 + core, ps)

    barrier = pltpu.get_barrier_semaphore()

    def greet(step, _):
        pl.semaphore_signal(barrier, inc=1, device_id=peer(step)[1], device_id_type=MESH)
        return 0

    lax.fori_loop(1, 128, greet, 0)
    pl.semaphore_signal(barrier, inc=1, device_id=partner, device_id_type=MESH)

    weights[0:128, :] = left_w[...].T
    weights[128:256, :] = right_w[...].T
    gain_col[...] = jnp.broadcast_to(mid_gain[...], (128, 128)).T

    def project(r, _):
        ao, bc = r // 3, r % 3
        v = x_ref[pl.ds(ao * 8, 8), pl.ds(pl.multiple_of(bc * 16, 16), 16), :].astype(F32).reshape(128, 128)
        v = v - jnp.mean(v, axis=1, keepdims=True)
        v = v * lax.rsqrt(jnp.mean(v * v, axis=1, keepdims=True) + 1e-05) * in_gain[...]
        v = v.astype(BF16)
        ready[r] = v
        both = lax.dot_general(weights[...], v, (((1,), (1,)), ((), ())), preferred_element_type=F32)
        wide[pl.ds(r, 128, stride=36), :] = both[0:128]
        wide[pl.ds(18 + r, 128, stride=36), :] = both[128:256]
        return 0

    lax.fori_loop(0, 18, project, 0)

    def pack(i, _):
        rows = pl.ds(pl.multiple_of(i * 128, 128), 128)
        sent[rows, :] = wide[rows, :].astype(BF16)
        return 0

    lax.fori_loop(0, 36, pack, 0)
    pl.semaphore_wait(barrier, 128)

    def send(step, _):
        chip, device = peer(step)
        pltpu.make_async_remote_copy(
            src_ref=sent.at[pl.ds(chip * 36, 36)],
            dst_ref=got.at[pl.ds(me * 36, 36)],
            send_sem=send_a,
            recv_sem=recv_a,
            device_id=device,
            device_id_type=MESH,
        ).start()
        return 0

    lax.fori_loop(1, 128, send, 0)

    def gate(r, _):
        g = jnp.dot(ready[r], gate_w[...], preferred_element_type=F32)
        gates[r] = jax.nn.sigmoid(g)
        return 0

    lax.fori_loop(0, 18, gate, 0)
    all_a = pl.ds(0, 127 * 36)
    pltpu.make_async_copy(sent.at[all_a], got.at[all_a], recv_a).wait()

    def unpack(i, _):
        rows = pl.ds(pl.multiple_of(i * 128, 128), 128)
        spread[rows, :] = got[rows, :].astype(F32)
        return 0

    lax.fori_loop(0, 36, unpack, 0)
    own = wide[pl.ds(me * 36, 36), :]
    spread[pl.ds(me * 36, 36), :] = own.astype(BF16).astype(F32)

    def gather(g, _):
        lanes = pl.ds(pl.multiple_of(g * 128, 128), 128)
        for side in range(2):
            pieces = []
            for ao in range(6):
                parts = []
                for p in range(8):
                    q = g * 8 + p
                    start = (q // 3) * 288 + q % 3 + side * 18 + ao * 3
                    parts.append(spread[pl.ds(start, 8, stride=36), :])
                parts = swap_blocks(parts)
                rows = jnp.concatenate(parts, axis=0).astype(BF16)
                if side == 1:
                    right[ao * 64 : ao * 64 + 64, lanes] = rows
                else:
                    pieces.append(rows)
                    if ao % 2 == 1:
                        block = jnp.concatenate(pieces, axis=0)
                        left[lanes, (ao // 2) * 128 : (ao // 2) * 128 + 128] = block.T
                        pieces = []
        return 0

    lax.fori_loop(0, 6, gather, 0)

    def multiply(t, _):
        rows = pl.ds(pl.multiple_of(t * 192, 64), 192)
        part = jnp.dot(left[rows, :], right[...], preferred_element_type=F32)
        for u in range(2):
            at = (t * 2 + u) * PITCH
            for g in range(6):
                sums[g, pl.ds(pl.multiple_of(at, 8), 96), :] = part[u * 96 : u * 96 + 96, g * 128 : g * 128 + 128]
        for u in range(2):
            zz = t * 2 + u
            pltpu.make_async_remote_copy(
                src_ref=sums.at[:, pl.ds(pl.multiple_of(zz * PITCH + (1 - core) * 48, 8), 48), :],
                dst_ref=other.at[:, pl.ds(pl.multiple_of(zz * HALF, 8), 48), :],
                send_sem=send_b.at[zz],
                recv_sem=recv_b.at[zz],
                device_id=partner,
                device_id_type=MESH,
            ).start()
        return 0

    lax.fori_loop(0, 4, multiply, 0)
    for i in range(8):
        pltpu.make_async_copy(
            sums.at[:, pl.ds(0, 48), :], other.at[:, pl.ds(0, 48), :], recv_b.at[i]
        ).wait()

    def scatter(g, _):
        for ao in range(6):
            parts = []
            for a8 in range(8):
                i = ao * 8 + a8
                mine = sums[g, pl.ds(core * 48 + i, 8, stride=PITCH), :]
                theirs = other[g, pl.ds(i, 8, stride=HALF), :]
                parts.append((mine + theirs) * 768 ** (-0.5))
            parts = swap_blocks(parts)
            for p in range(8):
                q = g * 8 + p
                start = (q // 3) * 144 + q % 3 + ao * 3
                wide2[pl.ds(start, 8, stride=18), :] = parts[p]
        return 0

    lax.fori_loop(0, 6, scatter, 0)

    def pack2(i, _):
        rows = pl.ds(pl.multiple_of(i * 128, 128), 128)
        sent2[rows, :] = wide2[rows, :].astype(BF16)
        return 0

    lax.fori_loop(0, 18, pack2, 0)

    def send2(step, _):
        chip, device = peer(step)
        pltpu.make_async_remote_copy(
            src_ref=sent2.at[pl.ds(chip * 18, 18)],
            dst_ref=got2.at[pl.ds(me * 18, 18)],
            send_sem=send_c,
            recv_sem=recv_c,
            device_id=device,
            device_id_type=MESH,
        ).start()
        return 0

    lax.fori_loop(1, 128, send2, 0)
    all_c = pl.ds(0, 127 * 18)
    pltpu.make_async_copy(sent2.at[all_c], got2.at[all_c], recv_c).wait()

    def unpack2(i, _):
        rows = pl.ds(pl.multiple_of(i * 128, 128), 128)
        spread2[rows, :] = got2[rows, :].astype(F32)
        return 0

    lax.fori_loop(0, 18, unpack2, 0)
    own2 = wide2[pl.ds(me * 18, 18), :]
    spread2[pl.ds(me * 18, 18), :] = own2.astype(BF16).astype(F32)

    def finish(r, _):
        ao, bc = r // 3, r % 3
        v = spread2[pl.ds(r, 128, stride=18), :]
        v = v - jnp.mean(v, axis=0, keepdims=True)
        v = v * lax.rsqrt(jnp.mean(v * v, axis=0, keepdims=True) + 1e-05) * gain_col[...]
        out = jnp.dot(v.astype(BF16).T, out_w[...], preferred_element_type=F32) * gates[r]
        o_ref[pl.ds(ao * 8, 8), pl.ds(pl.multiple_of(bc * 16, 16), 16), :] = out.astype(BF16).reshape(8, 16, 128)
        return 0

    lax.fori_loop(0, 18, finish, 0)
    pltpu.make_async_copy(sent.at[all_a], got.at[all_a], send_a).wait()
    for i in range(8):
        pltpu.make_async_copy(
            sums.at[:, pl.ds(0, 48), :], other.at[:, pl.ds(0, 48), :], send_b.at[i]
        ).wait()
    pltpu.make_async_copy(sent2.at[all_c], got2.at[all_c], send_c).wait()


def shards(pair_rows, in_gain, left_weight, right_weight, mid_gain, out_weight, out_gate):
    vmem = pl.BlockSpec(memory_space=pltpu.VMEM)
    return pl.pallas_call(
        kernel,
        out_shape=jax.ShapeDtypeStruct(pair_rows.shape, BF16),
        in_specs=[vmem] * 7,
        out_specs=vmem,
        scratch_shapes=[
            pltpu.VMEM((256, 128), BF16),
            pltpu.VMEM((18, 128, 128), BF16),
            pltpu.VMEM((128 * 36, 128), F32),
            pltpu.VMEM((128 * 36, 128), BF16),
            pltpu.VMEM((128 * 36, 128), BF16),
            pltpu.VMEM((128 * 36, 128), F32),
            pltpu.VMEM((768, 384), BF16),
            pltpu.VMEM((384, 768), BF16),
            pltpu.VMEM((6, 8 * PITCH, 128), F32),
            pltpu.VMEM((6, 8 * HALF, 128), F32),
            pltpu.VMEM((128 * 18, 128), F32),
            pltpu.VMEM((128 * 18, 128), BF16),
            pltpu.VMEM((128 * 18, 128), BF16),
            pltpu.VMEM((128 * 18, 128), F32),
            pltpu.VMEM((18, 128, 128), F32),
            pltpu.VMEM((128, 128), F32),
        ]
        + [pltpu.SemaphoreType.DMA] * 2
        + [pltpu.SemaphoreType.DMA((8,))] * 2
        + [pltpu.SemaphoreType.DMA] * 2,
        compiler_params=pltpu.CompilerParams(collective_id=0, has_side_effects=True),
    )(
        pair_rows, in_gain.reshape(1, 128), left_weight, right_weight,
        mid_gain.reshape(1, 128), out_weight, out_gate,
    )


def solution(mesh):
    in_specs = (P("first", "second", None), P(), P(), P(), P(), P(), P())
    out_specs = P("first", "second", None)
    return jax.shard_map(shards, mesh=mesh, in_specs=in_specs, out_specs=out_specs, check_vma=False)
```

```python
import jax
import jax.numpy as jnp
from jax import lax
from jax.experimental import pallas as pl
from jax.experimental.pallas import tpu as pltpu
from jax.sharding import PartitionSpec as P

MESH = pl.DeviceIdType.MESH
F32, BF16 = jnp.float32, jnp.bfloat16
PITCH = 24


def swap_blocks(parts):
    block = lax.broadcasted_iota(jnp.int32, parts[0].shape, 1) // 16
    for h in (4, 2, 1):
        low = (block // h) % 2 == 0
        out = list(parts)
        for p in range(8):
            if p // h % 2 == 0:
                a, b = parts[p], parts[p + h]
                out[p] = jnp.where(low, a, pltpu.roll(b, 16 * h, 1))
                out[p + h] = jnp.where(low, pltpu.roll(a, 128 - 16 * h, 1), b)
        parts = out
    return parts


def kernel(
    x_ref, in_gain, left_w, right_w, mid_gain, out_w, gate_w, o_ref,
    weights, ready, wide, sent, got, spread, left, right, sums, outgoing, other, wide2, sent2, got2, spread2, gates, gain_col,
    send_a, recv_a, send_b, recv_b, send_c, recv_c,
):
    first, second = lax.axis_index("first"), lax.axis_index("second")
    z, core, y, x = lax.div(first, 2), lax.rem(first, 2), lax.div(second, 4), lax.rem(second, 4)
    me = second * 8 + z
    partner = (first + 1 - 2 * core, second)
    columns = [lax.rem(x + dx, 4) for dx in (1, 2, 3, 0)]

    def each_peer(act):
        for dz in (4, 3, 5, 2, 6, 1, 7, 0):
            pz = lax.rem(z + dz, 8)

            def line(dy, _, pz=pz, count=4):
                row = lax.rem(y + dy, 4) * 4
                for column in columns[:count]:
                    ps = row + column
                    act(ps * 8 + pz, (pz * 2 + core, ps))
                return 0

            lax.fori_loop(1, 4, line, 0)
            line(0, 0, count=4 if dz else 3)

    barrier = pltpu.get_barrier_semaphore()
    each_peer(lambda chip, device: pl.semaphore_signal(barrier, inc=1, device_id=device, device_id_type=MESH))
    pl.semaphore_signal(barrier, inc=1, device_id=partner, device_id_type=MESH)

    weights[0] = left_w[...].T
    weights[1] = right_w[...].T
    gain_col[...] = jnp.broadcast_to(mid_gain[...], (128, 128)).T

    def turn(side, r, v):
        rows = lax.dot_general(weights[side], v, (((1,), (1,)), ((), ())), preferred_element_type=F32)
        wide[side, pl.ds(r, 128, stride=18), :] = rows

    def norm(r, _):
        ao, bc = lax.div(r, 3), lax.rem(r, 3)
        v = x_ref[pl.ds(ao * 8, 8), pl.ds(pl.multiple_of(bc * 16, 16), 16), :].astype(F32).reshape(128, 128)
        v = v - jnp.mean(v, axis=1, keepdims=True)
        v = v * lax.rsqrt(jnp.mean(v * v, axis=1, keepdims=True) + 1e-05) * in_gain[...]
        v = v.astype(BF16)
        ready[r] = v
        turn(1, r, v)
        return 0

    def project(r, _):
        turn(0, r, ready[r])
        return 0

    def pack(side):
        def step(i, _):
            rows = pl.ds(pl.multiple_of(i * 256, 256), 256)
            sent[side, rows, :] = wide[side, rows, :].astype(BF16)
            return 0

        lax.fori_loop(0, 9, step, 0)

    def send(side):
        def start(chip, device):
            pltpu.make_async_remote_copy(
                src_ref=sent.at[side, pl.ds(chip * 18, 18)],
                dst_ref=got.at[side, pl.ds(me * 18, 18)],
                send_sem=send_a.at[side],
                recv_sem=recv_a.at[side],
                device_id=device,
                device_id_type=MESH,
            ).start()

        each_peer(start)

    lax.fori_loop(0, 18, norm, 0, unroll=3)
    pack(1)
    pl.semaphore_wait(barrier, 128)
    send(1)
    lax.fori_loop(0, 18, project, 0, unroll=3)
    pack(0)
    send(0)

    def gate(r, _):
        g = jnp.dot(ready[r], gate_w[...], preferred_element_type=F32)
        gates[r] = jax.nn.sigmoid(g)
        return 0

    lax.fori_loop(0, 18, gate, 0, unroll=3)
    most = pl.ds(0, 127 * 18)

    def unpack(side):
        def step(i, _):
            rows = pl.ds(pl.multiple_of(i * 256, 256), 256)
            spread[side, rows, :] = got[side, rows, :].astype(F32)
            return 0

        lax.fori_loop(0, 9, step, 0)
        own = wide[side, pl.ds(me * 18, 18), :]
        spread[side, pl.ds(me * 18, 18), :] = own.astype(BF16).astype(F32)

    def gather_right(t, _):
        bc, h = lax.div(t, 2), lax.rem(t, 2)
        lanes = pl.ds(pl.multiple_of(t * 128, 128), 128)
        for ao in range(6):
            parts = [spread[1, pl.ds((h * 8 + p) * 144 + ao * 3 + bc, 8, stride=18), :] for p in range(8)]
            right[ao * 64 : ao * 64 + 64, lanes] = jnp.concatenate(swap_blocks(parts), axis=0).astype(BF16)
        return 0

    def gather_left(t, _):
        bc, h = lax.div(t, 2), lax.rem(t, 2)
        for pair in range(3):
            pieces = []
            for ao in (2 * pair, 2 * pair + 1):
                parts = [
                    spread[0, pl.ds((h * 8 + p % 4 * 2 + p // 4) * 144 + ao * 3 + bc, 8, stride=18), :]
                    for p in range(8)
                ]
                pieces += swap_blocks(parts)
            block = jnp.concatenate(pieces, axis=0).astype(BF16).T
            lanes = slice(pair * 128, pair * 128 + 128)
            left[pl.ds(pl.multiple_of((1 - core) * 384 + t * 64, 64), 64), lanes] = block[0:64]
            left[pl.ds(pl.multiple_of(core * 384 + t * 64, 64), 64), lanes] = block[64:128]
        return 0

    pltpu.make_async_copy(sent.at[1, most], got.at[1, most], recv_a.at[1]).wait()
    unpack(1)
    lax.fori_loop(0, 6, gather_right, 0)
    pltpu.make_async_copy(sent.at[0, most], got.at[0, most], recv_a.at[0]).wait()
    unpack(0)
    lax.fori_loop(0, 6, gather_left, 0)

    def product(target, half, bc):
        rows = pl.ds(pl.multiple_of(half * 384 + bc * 128, 128), 128)
        part = jnp.dot(left[rows, :], right[...], preferred_element_type=F32)
        for zz in range(8):
            for g in range(6):
                target[g, pl.ds(pl.multiple_of((bc * 8 + zz) * PITCH, 8), 16), :] = part[
                    zz * 16 : zz * 16 + 16, g * 128 : g * 128 + 128
                ]

    def multiply(bc, _):
        product(outgoing, 0, bc)
        for zz in range(8):
            rows = pl.ds(pl.multiple_of((bc * 8 + zz) * PITCH, 8), 16)
            pltpu.make_async_remote_copy(
                src_ref=outgoing.at[:, rows, :],
                dst_ref=other.at[:, rows, :],
                send_sem=send_b.at[bc],
                recv_sem=recv_b.at[bc],
                device_id=partner,
                device_id_type=MESH,
            ).start()
        return 0

    def multiply_own(bc, _):
        product(sums, 1, bc)
        return 0

    lax.fori_loop(0, 3, multiply, 0)
    lax.fori_loop(0, 3, multiply_own, 0)
    third = pl.ds(0, 128)

    def scatter(bc):
        def step(g, _):
            h, bd = lax.rem(g, 2), lax.div(g, 2)
            for ao in (2 * bc, 2 * bc + 1):
                parts = []
                for a8 in range(8):
                    rows = pl.ds(bc * 8 * PITCH + ao % 2 * 8 + a8, 8, stride=PITCH)
                    parts.append((sums[g, rows, :] + other[g, rows, :]) * 768 ** (-0.5))
                for p, part in enumerate(swap_blocks(parts)):
                    wide2[pl.ds((h * 8 + p) * 144 + ao * 3 + bd, 8, stride=18), :] = part
            return 0

        lax.fori_loop(0, 6, step, 0)

    for bc in range(3):
        pltpu.make_async_copy(outgoing.at[:, third, :], other.at[:, third, :], recv_b.at[bc]).wait()
        scatter(bc)

    def pack2(i, _):
        rows = pl.ds(pl.multiple_of(i * 256, 256), 256)
        sent2[rows, :] = wide2[rows, :].astype(BF16)
        return 0

    lax.fori_loop(0, 9, pack2, 0)

    def start2(chip, device):
        pltpu.make_async_remote_copy(
            src_ref=sent2.at[pl.ds(chip * 18, 18)],
            dst_ref=got2.at[pl.ds(me * 18, 18)],
            send_sem=send_c,
            recv_sem=recv_c,
            device_id=device,
            device_id_type=MESH,
        ).start()

    each_peer(start2)
    pltpu.make_async_copy(sent2.at[most], got2.at[most], recv_c).wait()

    def unpack2(i, _):
        rows = pl.ds(pl.multiple_of(i * 256, 256), 256)
        spread2[rows, :] = got2[rows, :].astype(F32)
        return 0

    lax.fori_loop(0, 9, unpack2, 0)
    own2 = wide2[pl.ds(me * 18, 18), :]
    spread2[pl.ds(me * 18, 18), :] = own2.astype(BF16).astype(F32)

    def finish(r, _):
        ao, bc = lax.div(r, 3), lax.rem(r, 3)
        v = spread2[pl.ds(r, 128, stride=18), :]
        v = v - jnp.mean(v, axis=0, keepdims=True)
        v = v * lax.rsqrt(jnp.mean(v * v, axis=0, keepdims=True) + 1e-05) * gain_col[...]
        out = jnp.dot(v.astype(BF16).T, out_w[...], preferred_element_type=F32) * gates[r]
        o_ref[pl.ds(ao * 8, 8), pl.ds(pl.multiple_of(bc * 16, 16), 16), :] = out.astype(BF16).reshape(8, 16, 128)
        return 0

    lax.fori_loop(0, 18, finish, 0, unroll=3)
    for side in range(2):
        pltpu.make_async_copy(sent.at[side, most], got.at[side, most], send_a.at[side]).wait()
    for bc in range(3):
        pltpu.make_async_copy(outgoing.at[:, third, :], other.at[:, third, :], send_b.at[bc]).wait()
    pltpu.make_async_copy(sent2.at[most], got2.at[most], send_c).wait()


def shards(pair_rows, in_gain, left_weight, right_weight, mid_gain, out_weight, out_gate):
    vmem = pl.BlockSpec(memory_space=pltpu.VMEM)
    return pl.pallas_call(
        kernel,
        out_shape=jax.ShapeDtypeStruct(pair_rows.shape, BF16),
        in_specs=[vmem] * 7,
        out_specs=vmem,
        scratch_shapes=[
            pltpu.VMEM((2, 128, 128), BF16),
            pltpu.VMEM((18, 128, 128), BF16),
            pltpu.VMEM((2, 128 * 18, 128), F32),
            pltpu.VMEM((2, 128 * 18, 128), BF16),
            pltpu.VMEM((2, 128 * 18, 128), BF16),
            pltpu.VMEM((2, 128 * 18, 128), F32),
            pltpu.VMEM((768, 384), BF16),
            pltpu.VMEM((384, 768), BF16),
            pltpu.VMEM((6, 24 * PITCH, 128), F32),
            pltpu.VMEM((6, 24 * PITCH, 128), F32),
            pltpu.VMEM((6, 24 * PITCH, 128), F32),
            pltpu.VMEM((128 * 18, 128), F32),
            pltpu.VMEM((128 * 18, 128), BF16),
            pltpu.VMEM((128 * 18, 128), BF16),
            pltpu.VMEM((128 * 18, 128), F32),
            pltpu.VMEM((18, 128, 128), F32),
            pltpu.VMEM((128, 128), F32),
            pltpu.SemaphoreType.DMA((2,)),
            pltpu.SemaphoreType.DMA((2,)),
            pltpu.SemaphoreType.DMA((3,)),
            pltpu.SemaphoreType.DMA((3,)),
            pltpu.SemaphoreType.DMA,
            pltpu.SemaphoreType.DMA,
        ],
        compiler_params=pltpu.CompilerParams(collective_id=0, has_side_effects=True),
    )(
        pair_rows, in_gain.reshape(1, 128), left_weight, right_weight,
        mid_gain.reshape(1, 128), out_weight, out_gate,
    )


def solution(mesh):
    in_specs = (P("first", "second", None), P(), P(), P(), P(), P(), P())
    out_specs = P("first", "second", None)
    return jax.shard_map(shards, mesh=mesh, in_specs=in_specs, out_specs=out_specs, check_vma=False)
```

```python
import jax
import jax.numpy as jnp
from jax import lax
from jax.experimental import pallas as pl
from jax.experimental.pallas import tpu as pltpu
from jax.sharding import PartitionSpec as P

MESH = pl.DeviceIdType.MESH
F32, BF16 = jnp.float32, jnp.bfloat16
PITCH = 24


def swap_blocks(parts):
    block = lax.broadcasted_iota(jnp.int32, parts[0].shape, 1) // 16
    for h in (4, 2, 1):
        low = (block // h) % 2 == 0
        out = list(parts)
        for p in range(8):
            if p // h % 2 == 0:
                a, b = parts[p], parts[p + h]
                out[p] = jnp.where(low, a, pltpu.roll(b, 16 * h, 1))
                out[p + h] = jnp.where(low, pltpu.roll(a, 128 - 16 * h, 1), b)
        parts = out
    return parts


def kernel(
    x_hbm, in_gain_hbm, left_hbm, right_hbm, mid_gain_hbm, out_hbm, gate_hbm, o_ref,
    x_ref, in_gain, left_w, right_w, mid_gain, out_w, gate_w,
    weights, ready, wide_r, wide_a, wide_b, sent_r, sent_a, sent_b, got_r, got_a, got_b,
    spread_r, spread_a, spread_b, left, right, sums, outgoing, other,
    wide2_a, wide2_b, sent2_a, sent2_b, got2_a, got2_b, spread2_a, spread2_b, gates, gain_col,
    load_sem, send_in, recv_in, send_swap, recv_swap, send_out, recv_out,
):
    first, second = lax.axis_index("first"), lax.axis_index("second")
    z, core, y, x = lax.div(first, 2), lax.rem(first, 2), lax.div(second, 4), lax.rem(second, 4)
    me = second * 8 + z
    partner = (first + 1 - 2 * core, second)
    columns = [lax.rem(x + dx, 4) for dx in (1, 2, 3, 0)]

    loads = [
        pltpu.make_async_copy(src, dst, load_sem.at[i])
        for i, (src, dst) in enumerate(
            [
                (x_hbm, x_ref), (right_hbm, right_w), (in_gain_hbm, in_gain), (left_hbm, left_w),
                (mid_gain_hbm, mid_gain), (out_hbm, out_w), (gate_hbm, gate_w),
            ]
        )
    ]
    for load in loads:
        load.start()

    def each_peer(act):
        for dz in (4, 3, 5, 2, 6, 1, 7, 0):
            pz = lax.rem(z + dz, 8)

            def line(dy, _, pz=pz, count=4):
                row = lax.rem(y + dy, 4) * 4
                for column in columns[:count]:
                    ps = row + column
                    act(ps * 8 + pz, (pz * 2 + core, ps))
                return 0

            lax.fori_loop(1, 4, line, 0)
            line(0, 0, count=4 if dz else 3)

    barrier = pltpu.get_barrier_semaphore()
    each_peer(lambda chip, device: pl.semaphore_signal(barrier, inc=1, device_id=device, device_id_type=MESH))
    pl.semaphore_signal(barrier, inc=1, device_id=partner, device_id_type=MESH)
    for load in loads:
        load.wait()

    weights[0] = left_w[...].T
    weights[1] = right_w[...].T
    gain_col[...] = jnp.broadcast_to(mid_gain[...], (128, 128)).T

    def turn(side, v):
        return lax.dot_general(weights[side], v, (((1,), (1,)), ((), ())), preferred_element_type=F32)

    def norm(r, _):
        ao, bc = lax.div(r, 3), lax.rem(r, 3)
        v = x_ref[pl.ds(ao * 8, 8), pl.ds(pl.multiple_of(bc * 16, 16), 16), :].astype(F32).reshape(128, 128)
        v = v - jnp.mean(v, axis=1, keepdims=True)
        v = v * lax.rsqrt(jnp.mean(v * v, axis=1, keepdims=True) + 1e-05) * in_gain[...]
        v = v.astype(BF16)
        ready[r] = v
        wide_r[pl.ds(r, 128, stride=18), :] = turn(1, v)
        return 0

    def project(ao, _):
        for bc in range(3):
            rows = turn(0, ready[ao * 3 + bc])
            if bc < 2:
                wide_a[pl.ds(bc * 6 + ao, 128, stride=12), :] = rows
            else:
                wide_b[pl.ds(ao, 128, stride=6), :] = rows
        return 0

    def convert(source, target):
        def step(i, _):
            rows = pl.ds(pl.multiple_of(i * 256, 256), 256)
            target[rows, :] = source[rows, :].astype(target.dtype)
            return 0

        lax.fori_loop(0, source.shape[0] // 256, step, 0)

    def send(source, target, send_sem, recv_sem):
        rows = source.shape[0] // 128

        def start(chip, device):
            pltpu.make_async_remote_copy(
                src_ref=source.at[pl.ds(chip * rows, rows)],
                dst_ref=target.at[pl.ds(me * rows, rows)],
                send_sem=send_sem,
                recv_sem=recv_sem,
                device_id=device,
                device_id_type=MESH,
            ).start()

        each_peer(start)

    def settle(source, target, sem):
        rows = pl.ds(0, source.shape[0] // 128 * 127)
        pltpu.make_async_copy(source.at[rows], target.at[rows], sem).wait()

    def receive(wide, source, target, spread, sem):
        settle(source, target, sem)
        convert(target, spread)
        rows = source.shape[0] // 128
        own = wide[pl.ds(me * rows, rows), :]
        spread[pl.ds(me * rows, rows), :] = own.astype(BF16).astype(F32)

    lax.fori_loop(0, 18, norm, 0, unroll=3)
    convert(wide_r, sent_r)
    pl.semaphore_wait(barrier, 128)
    send(sent_r, got_r, send_in.at[0], recv_in.at[0])
    lax.fori_loop(0, 6, project, 0)
    convert(wide_a, sent_a)
    send(sent_a, got_a, send_in.at[1], recv_in.at[1])
    convert(wide_b, sent_b)
    send(sent_b, got_b, send_in.at[2], recv_in.at[2])

    def gate(r, _):
        g = jnp.dot(ready[r], gate_w[...], preferred_element_type=F32)
        gates[r] = jax.nn.sigmoid(g)
        return 0

    lax.fori_loop(0, 18, gate, 0, unroll=3)

    def gather_right(t, _):
        bc, h = lax.div(t, 2), lax.rem(t, 2)
        lanes = pl.ds(pl.multiple_of(t * 128, 128), 128)
        for ao in range(6):
            parts = [spread_r[pl.ds((h * 8 + p) * 144 + ao * 3 + bc, 8, stride=18), :] for p in range(8)]
            right[ao * 64 : ao * 64 + 64, lanes] = jnp.concatenate(swap_blocks(parts), axis=0).astype(BF16)
        return 0

    def gather_left(spread, t, at):
        rows = spread.shape[0] // 128
        for pair in range(3):
            pieces = []
            for ao in (2 * pair, 2 * pair + 1):
                pieces += swap_blocks(
                    [
                        spread[pl.ds(at + (p % 4 * 2 + p // 4) * 8 * rows + ao, 8, stride=rows), :]
                        for p in range(8)
                    ]
                )
            block = jnp.concatenate(pieces, axis=0).astype(BF16).T
            lanes = slice(pair * 128, pair * 128 + 128)
            left[pl.ds(pl.multiple_of((1 - core) * 384 + t * 64, 64), 64), lanes] = block[0:64]
            left[pl.ds(pl.multiple_of(core * 384 + t * 64, 64), 64), lanes] = block[64:128]

    def gather_a(t, _):
        gather_left(spread_a, t, lax.rem(t, 2) * 768 + lax.div(t, 2) * 6)
        return 0

    def gather_b(h, _):
        gather_left(spread_b, 4 + h, h * 384)
        return 0

    def product(target, half, bc):
        rows = pl.ds(pl.multiple_of(half * 384 + bc * 128, 128), 128)
        part = jnp.dot(left[rows, :], right[...], preferred_element_type=F32)
        for zz in range(8):
            for g in range(6):
                target[g, pl.ds(pl.multiple_of((bc * 8 + zz) * PITCH, 8), 16), :] = part[
                    zz * 16 : zz * 16 + 16, g * 128 : g * 128 + 128
                ]

    def multiply(bc, _):
        product(outgoing, 0, bc)
        for zz in range(8):
            rows = pl.ds(pl.multiple_of((bc * 8 + zz) * PITCH, 8), 16)
            pltpu.make_async_remote_copy(
                src_ref=outgoing.at[:, rows, :],
                dst_ref=other.at[:, rows, :],
                send_sem=send_swap.at[bc],
                recv_sem=recv_swap.at[bc],
                device_id=partner,
                device_id_type=MESH,
            ).start()
        return 0

    def multiply_own(bc, _):
        product(sums, 1, bc)
        return 0

    third = pl.ds(0, 128)

    def scatter(wide, bc, skip):
        pltpu.make_async_copy(outgoing.at[:, third, :], other.at[:, third, :], recv_swap.at[bc]).wait()
        count = wide.shape[0] // 128

        def step(g, _):
            h, bd = lax.rem(g, 2), lax.div(g, 2)
            for ao in (2 * bc, 2 * bc + 1):
                parts = []
                for a8 in range(8):
                    rows = pl.ds(bc * 8 * PITCH + ao % 2 * 8 + a8, 8, stride=PITCH)
                    parts.append((sums[g, rows, :] + other[g, rows, :]) * 768 ** (-0.5))
                for p, part in enumerate(swap_blocks(parts)):
                    wide[pl.ds((h * 8 + p) * 8 * count + (ao - skip) * 3 + bd, 8, stride=count), :] = part
            return 0

        lax.fori_loop(0, 6, step, 0, unroll=2)

    def finish(spread, skip):
        def step(r, _):
            v = spread[pl.ds(r, 128, stride=spread.shape[0] // 128), :]
            v = v - jnp.mean(v, axis=0, keepdims=True)
            v = v * lax.rsqrt(jnp.mean(v * v, axis=0, keepdims=True) + 1e-05) * gain_col[...]
            out = jnp.dot(v.astype(BF16).T, out_w[...], preferred_element_type=F32) * gates[skip * 3 + r]
            ao, bc = skip + lax.div(r, 3), lax.rem(r, 3)
            o_ref[pl.ds(ao * 8, 8), pl.ds(pl.multiple_of(bc * 16, 16), 16), :] = out.astype(BF16).reshape(8, 16, 128)
            return 0

        lax.fori_loop(0, spread.shape[0] // 128, step, 0, unroll=3)

    receive(wide_r, sent_r, got_r, spread_r, recv_in.at[0])
    lax.fori_loop(0, 6, gather_right, 0)
    receive(wide_a, sent_a, got_a, spread_a, recv_in.at[1])
    lax.fori_loop(0, 4, gather_a, 0)
    lax.fori_loop(0, 2, multiply, 0)
    lax.fori_loop(0, 2, multiply_own, 0)
    scatter(wide2_a, 0, 0)
    scatter(wide2_a, 1, 0)
    convert(wide2_a, sent2_a)
    send(sent2_a, got2_a, send_out.at[0], recv_out.at[0])
    receive(wide_b, sent_b, got_b, spread_b, recv_in.at[2])
    lax.fori_loop(0, 2, gather_b, 0)
    multiply(2, 0)
    multiply_own(2, 0)
    scatter(wide2_b, 2, 4)
    convert(wide2_b, sent2_b)
    send(sent2_b, got2_b, send_out.at[1], recv_out.at[1])
    receive(wide2_a, sent2_a, got2_a, spread2_a, recv_out.at[0])
    finish(spread2_a, 0)
    receive(wide2_b, sent2_b, got2_b, spread2_b, recv_out.at[1])
    finish(spread2_b, 4)

    settle(sent_r, got_r, send_in.at[0])
    settle(sent_a, got_a, send_in.at[1])
    settle(sent_b, got_b, send_in.at[2])
    settle(sent2_a, got2_a, send_out.at[0])
    settle(sent2_b, got2_b, send_out.at[1])
    for bc in range(3):
        pltpu.make_async_copy(outgoing.at[:, third, :], other.at[:, third, :], send_swap.at[bc]).wait()


def shards(pair_rows, in_gain, left_weight, right_weight, mid_gain, out_weight, out_gate):
    hbm = pl.BlockSpec(memory_space=pltpu.HBM)
    square = pltpu.VMEM((128, 128), BF16)
    line = pltpu.VMEM((1, 128), F32)
    flat = [18, 12, 6]
    return pl.pallas_call(
        kernel,
        out_shape=pltpu.VMEM(pair_rows.shape, BF16),
        in_specs=[hbm] * 7,
        out_specs=pl.BlockSpec(memory_space=pltpu.VMEM),
        scratch_shapes=[
            pltpu.VMEM(pair_rows.shape, BF16), line, square, square, line, square, square,
            pltpu.VMEM((2, 128, 128), BF16),
            pltpu.VMEM((18, 128, 128), BF16),
        ]
        + [pltpu.VMEM((128 * n, 128), F32) for n in flat]
        + [pltpu.VMEM((128 * n, 128), BF16) for n in flat]
        + [pltpu.VMEM((128 * n, 128), BF16) for n in flat]
        + [pltpu.VMEM((128 * n, 128), F32) for n in flat]
        + [
            pltpu.VMEM((768, 384), BF16),
            pltpu.VMEM((384, 768), BF16),
            pltpu.VMEM((6, 24 * PITCH, 128), F32),
            pltpu.VMEM((6, 24 * PITCH, 128), F32),
            pltpu.VMEM((6, 24 * PITCH, 128), F32),
        ]
        + [pltpu.VMEM((128 * n, 128), F32) for n in flat[1:]]
        + [pltpu.VMEM((128 * n, 128), BF16) for n in flat[1:]]
        + [pltpu.VMEM((128 * n, 128), BF16) for n in flat[1:]]
        + [pltpu.VMEM((128 * n, 128), F32) for n in flat[1:]]
        + [
            pltpu.VMEM((18, 128, 128), F32),
            pltpu.VMEM((128, 128), F32),
        ]
        + [pltpu.SemaphoreType.DMA((n,)) for n in (7, 3, 3, 3, 3, 2, 2)],
        compiler_params=pltpu.CompilerParams(
            collective_id=0, has_side_effects=True
        ),
    )(
        pair_rows, in_gain.reshape(1, 128), left_weight, right_weight,
        mid_gain.reshape(1, 128), out_weight, out_gate,
    )


def solution(mesh):
    in_specs = (P("first", "second", None), P(), P(), P(), P(), P(), P())
    out_specs = P("first", "second", None)
    return jax.shard_map(shards, mesh=mesh, in_specs=in_specs, out_specs=out_specs, check_vma=False)
```

```python
import jax
import jax.numpy as jnp
from jax import lax
from jax.experimental import pallas as pl
from jax.experimental.pallas import tpu as pltpu
from jax.sharding import PartitionSpec as P

MESH = pl.DeviceIdType.MESH
F32, BF16 = jnp.float32, jnp.bfloat16
PITCH = 24


def swap_blocks(parts):
    block = lax.broadcasted_iota(jnp.int32, parts[0].shape, 1) // 16
    for h in (4, 2, 1):
        low = (block // h) % 2 == 0
        out = list(parts)
        for p in range(8):
            if p // h % 2 == 0:
                a, b = parts[p], parts[p + h]
                out[p] = jnp.where(low, a, pltpu.roll(b, 16 * h, 1))
                out[p + h] = jnp.where(low, pltpu.roll(a, 128 - 16 * h, 1), b)
        parts = out
    return parts


def kernel(
    x_hbm, in_gain_hbm, left_hbm, right_hbm, mid_gain_hbm, out_hbm, gate_hbm, o_ref,
    x_ref, in_gain, left_w, right_w, mid_gain, out_w, gate_w,
    weights, ready, wide_r, sent_r, got_r, spread_r, wide_l, sent_l, got_l, spread_l,
    left, right, sums, outgoing, other, wide_o, sent_o, got_o, spread_o, gates, gain_col,
    load_sem, send_in, recv_in, send_swap, recv_swap, send_out, recv_out,
):
    first, second = lax.axis_index("first"), lax.axis_index("second")
    z, core, y, x = lax.div(first, 2), lax.rem(first, 2), lax.div(second, 4), lax.rem(second, 4)
    me = second * 8 + z
    partner = (first + 1 - 2 * core, second)
    layers = [lax.rem(z + dz, 8) for dz in (0, 4, 1, 7, 2, 6, 3, 5)]

    loads = [
        pltpu.make_async_copy(src, dst, load_sem.at[i])
        for i, (src, dst) in enumerate(
            [
                (x_hbm, x_ref), (right_hbm, right_w), (in_gain_hbm, in_gain), (left_hbm, left_w),
                (mid_gain_hbm, mid_gain), (out_hbm, out_w), (gate_hbm, gate_w),
            ]
        )
    ]
    for load in loads:
        load.start()

    def each_peer(act):
        def ahead(i):
            return jnp.where(i == 0, 2, jnp.where(i == 1, 1, jnp.where(i == 2, 3, 0)))

        def column(e, _):
            ps = lax.rem(y + ahead(lax.div(e, 4)), 4) * 4 + lax.rem(x + ahead(lax.rem(e, 4)), 4)
            for pz in layers:
                act(ps * 8 + pz, (pz * 2 + core, ps))
            return 0

        lax.fori_loop(0, 15, column, 0)
        for pz in layers[1:]:
            act(second * 8 + pz, (pz * 2 + core, second))

    barrier = pltpu.get_barrier_semaphore()
    each_peer(lambda chip, device: pl.semaphore_signal(barrier, inc=1, device_id=device, device_id_type=MESH))
    pl.semaphore_signal(barrier, inc=1, device_id=partner, device_id_type=MESH)
    for load in loads:
        load.wait()

    weights[0] = left_w[...].T
    weights[1] = right_w[...].T
    gain_col[...] = jnp.broadcast_to(mid_gain[...], (128, 128)).T

    def turn(side, v):
        return lax.dot_general(weights[side], v, (((1,), (1,)), ((), ())), preferred_element_type=F32)

    def norm(r, _):
        ao, bc = lax.div(r, 3), lax.rem(r, 3)
        v = x_ref[pl.ds(ao * 8, 8), pl.ds(pl.multiple_of(bc * 16, 16), 16), :].astype(F32).reshape(128, 128)
        v = v - jnp.mean(v, axis=1, keepdims=True)
        v = v * lax.rsqrt(jnp.mean(v * v, axis=1, keepdims=True) + 1e-05) * in_gain[...]
        v = v.astype(BF16)
        ready[r] = v
        wide_r[pl.ds(r, 128, stride=18), :] = turn(1, v)
        return 0

    def project(ao, _):
        for bc in range(3):
            wide_l[bc, pl.ds(ao, 128, stride=6), :] = turn(0, ready[ao * 3 + bc])
        return 0

    def convert(source, target):
        def step(i, _):
            rows = pl.ds(pl.multiple_of(i * 256, 256), 256)
            target[rows, :] = source[rows, :].astype(target.dtype)
            return 0

        lax.fori_loop(0, source.shape[0] // 256, step, 0)

    def send(source, target, send_sem, recv_sem):
        rows = source.shape[0] // 128

        def start(chip, device):
            pltpu.make_async_remote_copy(
                src_ref=source.at[pl.ds(chip * rows, rows)],
                dst_ref=target.at[pl.ds(me * rows, rows)],
                send_sem=send_sem,
                recv_sem=recv_sem,
                device_id=device,
                device_id_type=MESH,
            ).start()

        each_peer(start)

    def settle(source, target, sem):
        rows = pl.ds(0, source.shape[0] // 128 * 127)
        pltpu.make_async_copy(source.at[rows], target.at[rows], sem).wait()

    def receive(wide, source, target, spread, sem):
        settle(source, target, sem)
        convert(target, spread)
        rows = source.shape[0] // 128
        own = wide[pl.ds(me * rows, rows), :]
        spread[pl.ds(me * rows, rows), :] = own.astype(BF16).astype(F32)

    lax.fori_loop(0, 18, norm, 0, unroll=3)
    convert(wide_r, sent_r)
    pl.semaphore_wait(barrier, 128)
    send(sent_r, got_r, send_in.at[0], recv_in.at[0])
    lax.fori_loop(0, 6, project, 0)

    def send_left(bc):
        convert(wide_l.at[bc], sent_l.at[bc])
        send(sent_l.at[bc], got_l.at[bc], send_in.at[1 + bc], recv_in.at[1 + bc])

    send_left(0)
    send_left(1)

    def gate(r, _):
        g = jnp.dot(ready[r], gate_w[...], preferred_element_type=F32)
        gates[r] = jax.nn.sigmoid(g)
        return 0

    lax.fori_loop(0, 18, gate, 0, unroll=3)

    def gather_right(t, _):
        bc, h = lax.div(t, 2), lax.rem(t, 2)
        lanes = pl.ds(pl.multiple_of(t * 128, 128), 128)
        for ao in range(6):
            parts = [spread_r[pl.ds((h * 8 + p) * 144 + ao * 3 + bc, 8, stride=18), :] for p in range(8)]
            right[ao * 64 : ao * 64 + 64, lanes] = jnp.concatenate(swap_blocks(parts), axis=0).astype(BF16)
        return 0

    def gather_left(t, _):
        bc, h = lax.div(t, 2), lax.rem(t, 2)
        for pair in range(3):
            pieces = []
            for ao in (2 * pair, 2 * pair + 1):
                pieces += swap_blocks(
                    [
                        spread_l[bc, pl.ds((h * 8 + p % 4 * 2 + p // 4) * 48 + ao, 8, stride=6), :]
                        for p in range(8)
                    ]
                )
            block = jnp.concatenate(pieces, axis=0).astype(BF16).T
            lanes = slice(pair * 128, pair * 128 + 128)
            left[pl.ds(pl.multiple_of((1 - core) * 384 + t * 64, 64), 64), lanes] = block[0:64]
            left[pl.ds(pl.multiple_of(core * 384 + t * 64, 64), 64), lanes] = block[64:128]
        return 0

    def product(target, half, bc):
        rows = pl.ds(pl.multiple_of(half * 384 + bc * 128, 128), 128)
        part = jnp.dot(left[rows, :], right[...], preferred_element_type=F32)
        for zz in range(8):
            for g in range(6):
                target[g, pl.ds(pl.multiple_of((bc * 8 + zz) * PITCH, 8), 16), :] = part[
                    zz * 16 : zz * 16 + 16, g * 128 : g * 128 + 128
                ]

    def multiply(bc):
        product(outgoing, 0, bc)
        for zz in range(8):
            rows = pl.ds((bc * 8 + zz) * PITCH, 16)
            pltpu.make_async_remote_copy(
                src_ref=outgoing.at[:, rows, :],
                dst_ref=other.at[:, rows, :],
                send_sem=send_swap.at[bc],
                recv_sem=recv_swap.at[bc],
                device_id=partner,
                device_id_type=MESH,
            ).start()
        product(sums, 1, bc)

    third = pl.ds(0, 128)

    def scatter(bc):
        pltpu.make_async_copy(outgoing.at[:, third, :], other.at[:, third, :], recv_swap.at[bc]).wait()

        def add(g, _):
            for zz in range(8):
                rows = pl.ds((bc * 8 + zz) * PITCH, 16)
                sums[g, rows, :] = (sums[g, rows, :] + other[g, rows, :]) * 768 ** (-0.5)
            return 0

        lax.fori_loop(0, 6, add, 0, unroll=2)

        def step(g, _):
            h, bd = lax.rem(g, 2), lax.div(g, 2)
            for ao in range(2):
                parts = [
                    sums[g, pl.ds(bc * 8 * PITCH + ao * 8 + a8, 8, stride=PITCH), :] for a8 in range(8)
                ]
                for p, part in enumerate(swap_blocks(parts)):
                    wide_o[bc, pl.ds((h * 8 + p) * 48 + ao * 3 + bd, 8, stride=6), :] = part
            return 0

        lax.fori_loop(0, 6, step, 0, unroll=3)

    def finish(part):
        def step(r, _):
            v = spread_o[part, pl.ds(r, 128, stride=6), :]
            v = v - jnp.mean(v, axis=0, keepdims=True)
            v = v * lax.rsqrt(jnp.mean(v * v, axis=0, keepdims=True) + 1e-05) * gain_col[...]
            out = jnp.dot(v.astype(BF16).T, out_w[...], preferred_element_type=F32) * gates[part * 6 + r]
            ao, bc = part * 2 + lax.div(r, 3), lax.rem(r, 3)
            o_ref[pl.ds(ao * 8, 8), pl.ds(pl.multiple_of(bc * 16, 16), 16), :] = out.astype(BF16).reshape(8, 16, 128)
            return 0

        lax.fori_loop(0, 6, step, 0, unroll=3)

    receive(wide_r, sent_r, got_r, spread_r, recv_in.at[0])
    send_left(2)
    lax.fori_loop(0, 6, gather_right, 0, unroll=2)
    for bc in range(3):
        receive(wide_l.at[bc], sent_l.at[bc], got_l.at[bc], spread_l.at[bc], recv_in.at[1 + bc])
        lax.fori_loop(2 * bc, 2 * bc + 2, gather_left, 0, unroll=2)
        multiply(bc)
        scatter(bc)
        convert(wide_o.at[bc], sent_o.at[bc])
        send(sent_o.at[bc], got_o.at[bc], send_out.at[bc], recv_out.at[bc])
    for part in range(3):
        receive(wide_o.at[part], sent_o.at[part], got_o.at[part], spread_o.at[part], recv_out.at[part])
        finish(part)

    settle(sent_r, got_r, send_in.at[0])
    for part in range(3):
        settle(sent_l.at[part], got_l.at[part], send_in.at[1 + part])
        settle(sent_o.at[part], got_o.at[part], send_out.at[part])
        pltpu.make_async_copy(outgoing.at[:, third, :], other.at[:, third, :], send_swap.at[part]).wait()


def shards(pair_rows, in_gain, left_weight, right_weight, mid_gain, out_weight, out_gate):
    hbm = pl.BlockSpec(memory_space=pltpu.HBM)
    square = pltpu.VMEM((128, 128), BF16)
    line = pltpu.VMEM((1, 128), F32)
    def flat(*parts):
        return [pltpu.VMEM(parts + (128,), dtype) for dtype in (F32, BF16, BF16, F32)]

    return pl.pallas_call(
        kernel,
        out_shape=pltpu.VMEM(pair_rows.shape, BF16),
        in_specs=[hbm] * 7,
        out_specs=pl.BlockSpec(memory_space=pltpu.VMEM),
        scratch_shapes=[
            pltpu.VMEM(pair_rows.shape, BF16), line, square, square, line, square, square,
            pltpu.VMEM((2, 128, 128), BF16),
            pltpu.VMEM((18, 128, 128), BF16),
        ]
        + flat(128 * 18)
        + flat(3, 128 * 6)
        + [
            pltpu.VMEM((768, 384), BF16),
            pltpu.VMEM((384, 768), BF16),
            pltpu.VMEM((6, 24 * PITCH, 128), F32),
            pltpu.VMEM((6, 24 * PITCH, 128), F32),
            pltpu.VMEM((6, 24 * PITCH, 128), F32),
        ]
        + flat(3, 128 * 6)
        + [
            pltpu.VMEM((18, 128, 128), F32),
            pltpu.VMEM((128, 128), F32),
        ]
        + [pltpu.SemaphoreType.DMA((n,)) for n in (7, 4, 4, 3, 3, 3, 3)],
        compiler_params=pltpu.CompilerParams(
            collective_id=0, has_side_effects=True
        ),
    )(
        pair_rows, in_gain.reshape(1, 128), left_weight, right_weight,
        mid_gain.reshape(1, 128), out_weight, out_gate,
    )


def solution(mesh):
    in_specs = (P("first", "second", None), P(), P(), P(), P(), P(), P())
    out_specs = P("first", "second", None)
    return jax.shard_map(shards, mesh=mesh, in_specs=in_specs, out_specs=out_specs, check_vma=False)
```

```python
import jax
import jax.numpy as jnp
from jax import lax
from jax.experimental import pallas as pl
from jax.experimental.pallas import tpu as pltpu
from jax.sharding import PartitionSpec as P

MESH = pl.DeviceIdType.MESH
F32, BF16 = jnp.float32, jnp.bfloat16
PITCH = 24


def swap_blocks(parts):
    block = lax.broadcasted_iota(jnp.int32, parts[0].shape, 1) // 16
    for h in (4, 2, 1):
        low = (block // h) % 2 == 0
        out = list(parts)
        for p in range(8):
            if p // h % 2 == 0:
                a, b = parts[p], parts[p + h]
                out[p] = jnp.where(low, a, pltpu.roll(b, 16 * h, 1))
                out[p + h] = jnp.where(low, pltpu.roll(a, 128 - 16 * h, 1), b)
        parts = out
    return parts


def kernel(
    x_hbm, in_gain_hbm, left_hbm, right_hbm, mid_gain_hbm, out_hbm, gate_hbm, o_ref,
    x_ref, in_gain, left_w, right_w, mid_gain, out_w, gate_w,
    weights, ready, wide_r, sent_r, got_r, spread_r, wide_l, sent_l, got_l, spread_l,
    left, right, left_in, right_in, sums, wide_o, sent_o, got_o, spread_o, gates, gain_col,
    load_sem, send_in, recv_in, send_swap, recv_swap, send_out, recv_out,
):
    first, second = lax.axis_index("first"), lax.axis_index("second")
    z, core, y, x = lax.div(first, 2), lax.rem(first, 2), lax.div(second, 4), lax.rem(second, 4)
    me = second * 8 + z
    partner = (first + 1 - 2 * core, second)
    layers = [lax.rem(z + dz, 8) for dz in (0, 4, 1, 7, 2, 6, 3, 5)]

    loads = [
        pltpu.make_async_copy(src, dst, load_sem.at[i])
        for i, (src, dst) in enumerate(
            [
                (x_hbm, x_ref), (right_hbm, right_w), (in_gain_hbm, in_gain), (left_hbm, left_w),
                (mid_gain_hbm, mid_gain), (out_hbm, out_w), (gate_hbm, gate_w),
            ]
        )
    ]
    for load in loads:
        load.start()

    def each_peer(act):
        def ahead(i):
            return jnp.where(i == 0, 2, jnp.where(i == 1, 1, jnp.where(i == 2, 3, 0)))

        def column(e, _):
            ps = lax.rem(y + ahead(lax.div(e, 4)), 4) * 4 + lax.rem(x + ahead(lax.rem(e, 4)), 4)
            for pz in layers:
                act(ps * 8 + pz, (pz * 2 + core, ps))
            return 0

        lax.fori_loop(0, 15, column, 0)
        for pz in layers[1:]:
            act(second * 8 + pz, (pz * 2 + core, second))

    barrier = pltpu.get_barrier_semaphore()
    each_peer(lambda chip, device: pl.semaphore_signal(barrier, inc=1, device_id=device, device_id_type=MESH))
    pl.semaphore_signal(barrier, inc=1, device_id=partner, device_id_type=MESH)
    for load in loads:
        load.wait()

    weights[0] = left_w[...].T
    weights[1] = right_w[...].T
    gain_col[...] = jnp.broadcast_to(mid_gain[...], (128, 128)).T

    def turn(side, v):
        return lax.dot_general(weights[side], v, (((1,), (1,)), ((), ())), preferred_element_type=F32)

    def norm(r, _):
        ao, bc = lax.div(r, 3), lax.rem(r, 3)
        v = x_ref[pl.ds(ao * 8, 8), pl.ds(pl.multiple_of(bc * 16, 16), 16), :].astype(F32).reshape(128, 128)
        v = v - jnp.mean(v, axis=1, keepdims=True)
        v = v * lax.rsqrt(jnp.mean(v * v, axis=1, keepdims=True) + 1e-05) * in_gain[...]
        v = v.astype(BF16)
        ready[r] = v
        wide_r[pl.ds(r, 128, stride=18), :] = turn(1, v)
        return 0

    def project(ao, _):
        for bc in range(3):
            wide_l[bc, pl.ds(ao, 128, stride=6), :] = turn(0, ready[ao * 3 + bc])
        return 0

    def convert(source, target):
        def step(i, _):
            rows = pl.ds(pl.multiple_of(i * 256, 256), 256)
            target[rows, :] = source[rows, :].astype(target.dtype)
            return 0

        lax.fori_loop(0, source.shape[0] // 256, step, 0)

    def send(source, target, send_sem, recv_sem):
        rows = source.shape[0] // 128

        def start(chip, device):
            pltpu.make_async_remote_copy(
                src_ref=source.at[pl.ds(chip * rows, rows)],
                dst_ref=target.at[pl.ds(me * rows, rows)],
                send_sem=send_sem,
                recv_sem=recv_sem,
                device_id=device,
                device_id_type=MESH,
            ).start()

        each_peer(start)

    def settle(source, target, sem):
        rows = pl.ds(0, source.shape[0] // 128 * 127)
        pltpu.make_async_copy(source.at[rows], target.at[rows], sem).wait()

    def receive(wide, source, target, spread, sem):
        settle(source, target, sem)
        convert(target, spread)
        rows = source.shape[0] // 128
        own = wide[pl.ds(me * rows, rows), :]
        spread[pl.ds(me * rows, rows), :] = own.astype(BF16).astype(F32)

    lax.fori_loop(0, 18, norm, 0, unroll=3)
    convert(wide_r, sent_r)
    pl.semaphore_wait(barrier, 128)
    send(sent_r, got_r, send_in.at[0], recv_in.at[0])
    lax.fori_loop(0, 6, project, 0)

    def send_left(bc):
        convert(wide_l.at[bc], sent_l.at[bc])
        send(sent_l.at[bc], got_l.at[bc], send_in.at[1 + bc], recv_in.at[1 + bc])

    send_left(0)
    send_left(1)

    def gate(r, _):
        g = jnp.dot(ready[r], gate_w[...], preferred_element_type=F32)
        gates[r] = jax.nn.sigmoid(g)
        return 0

    lax.fori_loop(0, 18, gate, 0, unroll=3)

    def gather_right(t, _):
        bc, h = lax.div(t, 2), lax.rem(t, 2)
        lanes = pl.ds(pl.multiple_of(t * 128, 128), 128)
        for ao in range(6):
            parts = [spread_r[pl.ds((h * 8 + p) * 144 + ao * 3 + bc, 8, stride=18), :] for p in range(8)]
            right[ao * 64 : ao * 64 + 64, lanes] = jnp.concatenate(swap_blocks(parts), axis=0).astype(BF16)
        return 0

    def gather_left(t, _):
        bc, h = lax.div(t, 2), lax.rem(t, 2)
        for pair in range(3):
            pieces = []
            for ao in (2 * pair, 2 * pair + 1):
                pieces += swap_blocks(
                    [
                        spread_l[bc, pl.ds((h * 8 + p % 4 * 2 + p // 4) * 48 + ao, 8, stride=6), :]
                        for p in range(8)
                    ]
                )
            block = jnp.concatenate(pieces, axis=0).astype(BF16).T
            lanes = slice(pair * 128, pair * 128 + 128)
            left[pl.ds(pl.multiple_of((1 - core) * 384 + t * 64, 64), 64), lanes] = block[0:64]
            left[pl.ds(pl.multiple_of(core * 384 + t * 64, 64), 64), lanes] = block[64:128]
        return 0

    def swap(source, target, at, i):
        rows = pl.ds(at, target.shape[0])
        return pltpu.make_async_remote_copy(
            src_ref=source.at[rows, :],
            dst_ref=target,
            send_sem=send_swap.at[i],
            recv_sem=recv_swap.at[i],
            device_id=partner,
            device_id_type=MESH,
        )

    def multiply(bc):
        given = swap(left, left_in.at[pl.ds(bc * 128, 128), :], bc * 128, bc)
        given.start()
        part = jnp.dot(left[384 + bc * 128 : 512 + bc * 128, :], right[...], preferred_element_type=F32)
        for zz in range(8):
            for g in range(6):
                sums[g, (bc * 8 + zz) * PITCH : (bc * 8 + zz) * PITCH + 16, :] = part[
                    zz * 16 : zz * 16 + 16, g * 128 : g * 128 + 128
                ]
        if bc == 0:
            swap(right, right_in, 0, 3).wait_recv()
        given.wait_recv()
        part = jnp.dot(left_in[bc * 128 : bc * 128 + 128, :], right_in[...], preferred_element_type=F32)
        for zz in range(8):
            for g in range(6):
                rows = slice((bc * 8 + zz) * PITCH, (bc * 8 + zz) * PITCH + 16)
                sums[g, rows, :] = (
                    sums[g, rows, :] + part[zz * 16 : zz * 16 + 16, g * 128 : g * 128 + 128]
                ) * 768 ** (-0.5)

    def scatter(bc):
        def step(g, _):
            h, bd = lax.rem(g, 2), lax.div(g, 2)
            for ao in range(2):
                parts = [
                    sums[g, pl.ds(bc * 8 * PITCH + ao * 8 + a8, 8, stride=PITCH), :] for a8 in range(8)
                ]
                for p, part in enumerate(swap_blocks(parts)):
                    wide_o[bc, pl.ds((h * 8 + p) * 48 + ao * 3 + bd, 8, stride=6), :] = part
            return 0

        lax.fori_loop(0, 6, step, 0, unroll=3)

    def finish(part):
        def step(r, _):
            v = spread_o[part, pl.ds(r, 128, stride=6), :]
            v = v - jnp.mean(v, axis=0, keepdims=True)
            v = v * lax.rsqrt(jnp.mean(v * v, axis=0, keepdims=True) + 1e-05) * gain_col[...]
            out = jnp.dot(v.astype(BF16).T, out_w[...], preferred_element_type=F32) * gates[part * 6 + r]
            ao, bc = part * 2 + lax.div(r, 3), lax.rem(r, 3)
            o_ref[pl.ds(ao * 8, 8), pl.ds(pl.multiple_of(bc * 16, 16), 16), :] = out.astype(BF16).reshape(8, 16, 128)
            return 0

        lax.fori_loop(0, 6, step, 0, unroll=6)

    receive(wide_r, sent_r, got_r, spread_r, recv_in.at[0])
    send_left(2)
    lax.fori_loop(0, 6, gather_right, 0, unroll=2)
    swap(right, right_in, 0, 3).start()
    for bc in range(3):
        receive(wide_l.at[bc], sent_l.at[bc], got_l.at[bc], spread_l.at[bc], recv_in.at[1 + bc])
        lax.fori_loop(2 * bc, 2 * bc + 2, gather_left, 0, unroll=2)
        multiply(bc)
        scatter(bc)
        convert(wide_o.at[bc], sent_o.at[bc])
        send(sent_o.at[bc], got_o.at[bc], send_out.at[bc], recv_out.at[bc])
    for part in range(3):
        receive(wide_o.at[part], sent_o.at[part], got_o.at[part], spread_o.at[part], recv_out.at[part])
        finish(part)

    settle(sent_r, got_r, send_in.at[0])
    for part in range(3):
        settle(sent_l.at[part], got_l.at[part], send_in.at[1 + part])
        settle(sent_o.at[part], got_o.at[part], send_out.at[part])
        swap(left, left_in.at[pl.ds(part * 128, 128), :], part * 128, part).wait_send()
    swap(right, right_in, 0, 3).wait_send()


def shards(pair_rows, in_gain, left_weight, right_weight, mid_gain, out_weight, out_gate):
    hbm = pl.BlockSpec(memory_space=pltpu.HBM)
    square = pltpu.VMEM((128, 128), BF16)
    line = pltpu.VMEM((1, 128), F32)
    def flat(*parts):
        return [pltpu.VMEM(parts + (128,), dtype) for dtype in (F32, BF16, BF16, F32)]

    return pl.pallas_call(
        kernel,
        out_shape=pltpu.VMEM(pair_rows.shape, BF16),
        in_specs=[hbm] * 7,
        out_specs=pl.BlockSpec(memory_space=pltpu.VMEM),
        scratch_shapes=[
            pltpu.VMEM(pair_rows.shape, BF16), line, square, square, line, square, square,
            pltpu.VMEM((2, 128, 128), BF16),
            pltpu.VMEM((18, 128, 128), BF16),
        ]
        + flat(128 * 18)
        + flat(3, 128 * 6)
        + [
            pltpu.VMEM((768, 384), BF16),
            pltpu.VMEM((384, 768), BF16),
            pltpu.VMEM((384, 384), BF16),
            pltpu.VMEM((384, 768), BF16),
            pltpu.VMEM((6, 24 * PITCH, 128), F32),
        ]
        + flat(3, 128 * 6)
        + [
            pltpu.VMEM((18, 128, 128), F32),
            pltpu.VMEM((128, 128), F32),
        ]
        + [pltpu.SemaphoreType.DMA((n,)) for n in (7, 4, 4, 4, 4, 3, 3)],
        compiler_params=pltpu.CompilerParams(
            collective_id=0, has_side_effects=True
        ),
    )(
        pair_rows, in_gain.reshape(1, 128), left_weight, right_weight,
        mid_gain.reshape(1, 128), out_weight, out_gate,
    )


def solution(mesh):
    in_specs = (P("first", "second", None), P(), P(), P(), P(), P(), P())
    out_specs = P("first", "second", None)
    return jax.shard_map(shards, mesh=mesh, in_specs=in_specs, out_specs=out_specs, check_vma=False)
```

```python
import jax
import jax.numpy as jnp
from jax import lax
from jax.experimental import pallas as pl
from jax.experimental.pallas import tpu as pltpu
from jax.sharding import PartitionSpec as P

MESH = pl.DeviceIdType.MESH
F32, BF16 = jnp.float32, jnp.bfloat16
PITCH = 24


def swap_blocks(parts):
    block = lax.broadcasted_iota(jnp.int32, parts[0].shape, 1) // 16
    for h in (4, 2, 1):
        low = (block // h) % 2 == 0
        out = list(parts)
        for p in range(8):
            if p // h % 2 == 0:
                a, b = parts[p], parts[p + h]
                out[p] = jnp.where(low, a, pltpu.roll(b, 16 * h, 1))
                out[p + h] = jnp.where(low, pltpu.roll(a, 128 - 16 * h, 1), b)
        parts = out
    return parts


def kernel(
    x_hbm, in_gain_hbm, left_hbm, right_hbm, mid_gain_hbm, out_hbm, gate_hbm, o_ref,
    x_ref, in_gain, left_w, right_w, mid_gain, out_w, gate_w,
    weights, ready, wide_r, sent_r, got_r, spread_r, wide_l, sent_l, got_l, spread_l,
    left, right, outbox, inbox, sums, wide_o, sent_o, got_o, spread_o, gates, gain_col,
    load_sem, send_in, recv_in, send_swap, recv_swap, send_out, recv_out,
):
    first, second = lax.axis_index("first"), lax.axis_index("second")
    z, core, y, x = lax.div(first, 2), lax.rem(first, 2), lax.div(second, 4), lax.rem(second, 4)
    a_own = lax.rem(z + 8 - core, 8)
    partner = (lax.rem(z + 1 + 6 * core, 8) * 2 + 1 - core, second)
    mine = [lax.rem(z + 5 - 5 * core + j, 8) for j in range(4)]
    theirs = [lax.rem(z + 1 + 3 * core + j, 8) for j in range(4)]
    near = [lax.rem(z + d, 8) for d in range(8)]

    loads = [
        pltpu.make_async_copy(src, dst, load_sem.at[i])
        for i, (src, dst) in enumerate(
            [
                (x_hbm, x_ref), (right_hbm, right_w), (in_gain_hbm, in_gain), (left_hbm, left_w),
                (mid_gain_hbm, mid_gain), (out_hbm, out_w), (gate_hbm, gate_w),
            ]
        )
    ]
    for load in loads:
        load.start()

    def each_column(act):
        def ahead(i):
            return jnp.where(i == 0, 2, jnp.where(i == 1, 1, jnp.where(i == 2, 3, 0)))

        def step(e, _):
            act(lax.rem(y + ahead(lax.div(e, 4)), 4) * 4 + lax.rem(x + ahead(lax.rem(e, 4)), 4), False)
            return 0

        lax.fori_loop(0, 15, step, 0)
        act(second, True)

    barrier = pltpu.get_barrier_semaphore()

    def greet(column, is_own):
        targets = [(near[d], core) for d in (-3, 3, -2, 2, -1, 1)] + ([] if is_own else [(z, core)])
        for layer, c in targets + [(layer, 1 - core) for layer in mine]:
            pl.semaphore_signal(barrier, inc=1, device_id=(layer * 2 + c, column), device_id_type=MESH)

    each_column(greet)
    pl.semaphore_signal(barrier, inc=1, device_id=partner, device_id_type=MESH)
    for load in loads:
        load.wait()

    weights[0] = left_w[...].T
    weights[1] = right_w[...].T
    gain_col[...] = jnp.broadcast_to(mid_gain[...], (128, 128)).T

    def turn(side, v):
        return lax.dot_general(weights[side], v, (((1,), (1,)), ((), ())), preferred_element_type=F32)

    def norm(r, _):
        ao, bc = lax.div(r, 3), lax.rem(r, 3)
        v = x_ref[pl.ds(ao * 8, 8), pl.ds(pl.multiple_of(bc * 16, 16), 16), :].astype(F32).reshape(128, 128)
        v = v - jnp.mean(v, axis=1, keepdims=True)
        v = v * lax.rsqrt(jnp.mean(v * v, axis=1, keepdims=True) + 1e-05) * in_gain[...]
        v = v.astype(BF16)
        ready[r] = v
        wide_r[pl.ds(r, 128, stride=18), :] = turn(1, v)
        return 0

    def project(ao, _):
        for bc in range(3):
            wide_l[bc, pl.ds(ao, 128, stride=6), :] = turn(0, ready[ao * 3 + bc])
        return 0

    def convert(source, target):
        def step(i, _):
            rows = pl.ds(pl.multiple_of(i * 256, 256), 256)
            target[rows, :] = source[rows, :].astype(target.dtype)
            return 0

        lax.fori_loop(0, source.shape[0] // 256, step, 0)

    def start(source, target, send_sem, recv_sem, chunk, slot, device):
        rows = source.shape[0] // 128
        pltpu.make_async_remote_copy(
            src_ref=source.at[pl.ds(chunk * rows, rows)],
            dst_ref=target.at[pl.ds(slot * rows, rows)],
            send_sem=send_sem,
            recv_sem=recv_sem,
            device_id=device,
            device_id_type=MESH,
        ).start()

    def send(*refs):
        def act(column, is_own):
            for o in (7, 3, 4, 0, 2, 5, 1, 6):
                layer, c = (near[o], 0) if o < 4 else (near[(o + 1) % 8], 1)
                args = (column * 8 + near[o], second * 8 + o % 4 * 2 + core, (layer * 2 + c, column))
                if is_own and o in (0, 7):
                    pl.when(core == (1 if o == 0 else 0))(lambda args=args: start(*refs, *args))
                else:
                    start(*refs, *args)

        each_column(act)

    def send_back(*refs):
        def act(column, is_own):
            for p in (0, 6, 2, 5, 1, 7, 3, 4):
                args = (column * 8 + p, second * 8 + a_own, (mine[p // 2] * 2 + p % 2, column))
                if is_own and p in (1, 6):
                    pl.when(core == (1 if p == 6 else 0))(lambda args=args: start(*refs, *args))
                else:
                    start(*refs, *args)

        each_column(act)

    def settle(source, target, sem):
        rows = pl.ds(0, source.shape[0] // 128 * 127)
        pltpu.make_async_copy(source.at[rows], target.at[rows], sem).wait()

    def receive(wide, source, target, spread, sem, chunk, slot):
        settle(source, target, sem)
        convert(target, spread)
        rows = source.shape[0] // 128
        own = wide[pl.ds((second * 8 + chunk) * rows, rows), :]
        spread[pl.ds((second * 8 + slot) * rows, rows), :] = own.astype(BF16).astype(F32)

    lax.fori_loop(0, 18, norm, 0, unroll=3)
    convert(wide_r, sent_r)
    pl.semaphore_wait(barrier, 176)
    send(sent_r, got_r, send_in.at[0], recv_in.at[0])
    lax.fori_loop(0, 6, project, 0)

    def send_left(bc):
        convert(wide_l.at[bc], sent_l.at[bc])
        send(sent_l.at[bc], got_l.at[bc], send_in.at[1 + bc], recv_in.at[1 + bc])

    send_left(0)
    send_left(1)

    def gate(r, _):
        g = jnp.dot(ready[r], gate_w[...], preferred_element_type=F32)
        gates[r] = jax.nn.sigmoid(g)
        return 0

    lax.fori_loop(0, 18, gate, 0, unroll=3)

    def gather_right(t, _):
        bc, h = lax.div(t, 2), lax.rem(t, 2)
        lanes = pl.ds(pl.multiple_of(t * 128, 128), 128)
        for ao in range(6):
            parts = [spread_r[pl.ds((h * 8 + p) * 144 + ao * 3 + bc, 8, stride=18), :] for p in range(8)]
            right[ao * 64 : ao * 64 + 64, lanes] = jnp.concatenate(swap_blocks(parts), axis=0).astype(BF16)
        return 0

    def gather_left(bc):
        for half, layers in enumerate((theirs, mine)):
            for pair in range(3):
                pieces = []
                for ao in (2 * pair, 2 * pair + 1):
                    pieces += swap_blocks(
                        [
                            spread_l[bc, pl.ds((layers[p // 2] * 2 + p % 2) * 48 + ao, 8, stride=6), :]
                            for p in range(8)
                        ]
                    )
                block = jnp.concatenate(pieces, axis=0).astype(BF16)
                left[bc, half * 128 : half * 128 + 128, pair * 128 : pair * 128 + 128] = block.T

    def swap(bc):
        return pltpu.make_async_remote_copy(
            src_ref=outbox.at[bc],
            dst_ref=inbox.at[bc],
            send_sem=send_swap.at[bc],
            recv_sem=recv_swap.at[bc],
            device_id=partner,
            device_id_type=MESH,
        )

    def multiply(bc):
        outbox[bc] = jnp.dot(left[bc, 0:128, :], right[...], preferred_element_type=F32).astype(BF16)
        swap(bc).start()
        part = jnp.dot(left[bc, 128:256, :], right[...], preferred_element_type=F32)
        for zz in range(8):
            for g in range(6):
                sums[g, (bc * 8 + zz) * PITCH : (bc * 8 + zz) * PITCH + 16, :] = part[
                    zz * 16 : zz * 16 + 16, g * 128 : g * 128 + 128
                ]

    def scatter(bc):
        swap(bc).wait_recv()
        for zz in range(8):
            for g in range(6):
                rows = slice((bc * 8 + zz) * PITCH, (bc * 8 + zz) * PITCH + 16)
                there = inbox[bc, zz * 16 : zz * 16 + 16, g * 128 : g * 128 + 128].astype(F32)
                sums[g, rows, :] = (sums[g, rows, :] + there) * 768 ** (-0.5)

        def step(g, _):
            h, bd = lax.rem(g, 2), lax.div(g, 2)
            for ao in range(2):
                parts = [
                    sums[g, pl.ds(bc * 8 * PITCH + ao * 8 + a8, 8, stride=PITCH), :] for a8 in range(8)
                ]
                for p, part in enumerate(swap_blocks(parts)):
                    wide_o[bc, pl.ds((h * 8 + p) * 48 + ao * 3 + bd, 8, stride=6), :] = part
            return 0

        lax.fori_loop(0, 6, step, 0, unroll=3)

    def finish(part):
        def step(r, _):
            v = spread_o[part, pl.ds(r, 128, stride=6), :]
            v = v - jnp.mean(v, axis=0, keepdims=True)
            v = v * lax.rsqrt(jnp.mean(v * v, axis=0, keepdims=True) + 1e-05) * gain_col[...]
            out = jnp.dot(v.astype(BF16).T, out_w[...], preferred_element_type=F32) * gates[part * 6 + r]
            ao, bc = part * 2 + lax.div(r, 3), lax.rem(r, 3)
            o_ref[pl.ds(ao * 8, 8), pl.ds(pl.multiple_of(bc * 16, 16), 16), :] = out.astype(BF16).reshape(8, 16, 128)
            return 0

        lax.fori_loop(0, 6, step, 0, unroll=6)

    def take(bc):
        receive(wide_l.at[bc], sent_l.at[bc], got_l.at[bc], spread_l.at[bc], recv_in.at[1 + bc], a_own, core * 7)
        gather_left(bc)
        multiply(bc)

    def give(bc):
        scatter(bc)
        convert(wide_o.at[bc], sent_o.at[bc])
        send_back(sent_o.at[bc], got_o.at[bc], send_out.at[bc], recv_out.at[bc])

    receive(wide_r, sent_r, got_r, spread_r, recv_in.at[0], a_own, core * 7)
    send_left(2)
    lax.fori_loop(0, 6, gather_right, 0, unroll=2)
    take(0)
    take(1)
    give(0)
    take(2)
    give(1)
    give(2)
    for part in range(3):
        receive(
            wide_o.at[part], sent_o.at[part], got_o.at[part], spread_o.at[part], recv_out.at[part],
            6 - 5 * core, a_own,
        )
        finish(part)

    settle(sent_r, got_r, send_in.at[0])
    for part in range(3):
        settle(sent_l.at[part], got_l.at[part], send_in.at[1 + part])
        settle(sent_o.at[part], got_o.at[part], send_out.at[part])
        swap(part).wait_send()


def shards(pair_rows, in_gain, left_weight, right_weight, mid_gain, out_weight, out_gate):
    hbm = pl.BlockSpec(memory_space=pltpu.HBM)
    square = pltpu.VMEM((128, 128), BF16)
    line = pltpu.VMEM((1, 128), F32)
    def flat(*parts):
        return [pltpu.VMEM(parts + (128,), dtype) for dtype in (F32, BF16, BF16, F32)]

    return pl.pallas_call(
        kernel,
        out_shape=pltpu.VMEM(pair_rows.shape, BF16),
        in_specs=[hbm] * 7,
        out_specs=pl.BlockSpec(memory_space=pltpu.VMEM),
        scratch_shapes=[
            pltpu.VMEM(pair_rows.shape, BF16), line, square, square, line, square, square,
            pltpu.VMEM((2, 128, 128), BF16),
            pltpu.VMEM((18, 128, 128), BF16),
        ]
        + flat(128 * 18)
        + flat(3, 128 * 6)
        + [
            pltpu.VMEM((3, 256, 384), BF16),
            pltpu.VMEM((384, 768), BF16),
            pltpu.VMEM((3, 128, 768), BF16),
            pltpu.VMEM((3, 128, 768), BF16),
            pltpu.VMEM((6, 24 * PITCH, 128), F32),
        ]
        + flat(3, 128 * 6)
        + [
            pltpu.VMEM((18, 128, 128), F32),
            pltpu.VMEM((128, 128), F32),
        ]
        + [pltpu.SemaphoreType.DMA((n,)) for n in (7, 4, 4, 3, 3, 3, 3)],
        compiler_params=pltpu.CompilerParams(
            collective_id=0, has_side_effects=True
        ),
    )(
        pair_rows, in_gain.reshape(1, 128), left_weight, right_weight,
        mid_gain.reshape(1, 128), out_weight, out_gate,
    )


def solution(mesh):
    in_specs = (P("first", "second", None), P(), P(), P(), P(), P(), P())
    out_specs = P("first", "second", None)
    return jax.shard_map(shards, mesh=mesh, in_specs=in_specs, out_specs=out_specs, check_vma=False)
```

```python
import jax
import jax.numpy as jnp
from jax import lax
from jax.experimental import pallas as pl
from jax.experimental.pallas import tpu as pltpu
from jax.sharding import PartitionSpec as P

MESH = pl.DeviceIdType.MESH
F32, BF16 = jnp.float32, jnp.bfloat16
PITCH = 24


def swap_blocks(parts):
    block = lax.broadcasted_iota(jnp.int32, parts[0].shape, 1) // 16
    for h in (4, 2, 1):
        low = (block // h) % 2 == 0
        out = list(parts)
        for p in range(8):
            if p // h % 2 == 0:
                a, b = parts[p], parts[p + h]
                out[p] = jnp.where(low, a, pltpu.roll(b, 16 * h, 1))
                out[p + h] = jnp.where(low, pltpu.roll(a, 128 - 16 * h, 1), b)
        parts = out
    return parts


def kernel(
    x_hbm, in_gain_hbm, left_hbm, right_hbm, mid_gain_hbm, out_hbm, gate_hbm, o_ref,
    x_ref, in_gain, left_w, right_w, mid_gain, out_w, gate_w,
    weights, ready, wide_r, sent_r, got_r, spread_r, wide_l, sent_l, got_l, spread_l,
    left, right, outbox, inbox, sums, wide_o, sent_o, got_o, spread_o, gates, gain_col,
    load_sem, send_in, recv_in, send_swap, recv_swap, send_out, recv_out,
):
    first, second = lax.axis_index("first"), lax.axis_index("second")
    z, core, y, x = lax.div(first, 2), lax.rem(first, 2), lax.div(second, 4), lax.rem(second, 4)
    a_own = lax.rem(z + 8 - core, 8)
    partner = (lax.rem(z + 1 + 6 * core, 8) * 2 + 1 - core, second)
    mine = [lax.rem(z + 5 - 5 * core + j, 8) for j in range(4)]
    theirs = [lax.rem(z + 1 + 3 * core + j, 8) for j in range(4)]
    near = [lax.rem(z + d, 8) for d in range(8)]

    loads = [
        pltpu.make_async_copy(src, dst, load_sem.at[i])
        for i, (src, dst) in enumerate(
            [
                (x_hbm, x_ref), (right_hbm, right_w), (in_gain_hbm, in_gain), (left_hbm, left_w),
                (mid_gain_hbm, mid_gain), (out_hbm, out_w), (gate_hbm, gate_w),
            ]
        )
    ]
    for load in loads:
        load.start()

    def each_column(act):
        def ahead(i):
            return jnp.where(i == 0, 2, jnp.where(i == 1, 1, jnp.where(i == 2, 3, 0)))

        def step(e, _):
            act(lax.rem(y + ahead(lax.div(e, 4)), 4) * 4 + lax.rem(x + ahead(lax.rem(e, 4)), 4), False)
            return 0

        lax.fori_loop(0, 15, step, 0)
        act(second, True)

    barrier = pltpu.get_barrier_semaphore()

    def greet(column, is_own):
        targets = [(near[d], core) for d in (-3, 3, -2, 2, -1, 1)] + ([] if is_own else [(z, core)])
        for layer, c in targets + [(layer, 1 - core) for layer in mine]:
            pl.semaphore_signal(barrier, inc=1, device_id=(layer * 2 + c, column), device_id_type=MESH)

    each_column(greet)
    pl.semaphore_signal(barrier, inc=1, device_id=partner, device_id_type=MESH)
    for load in loads:
        load.wait()

    weights[0] = left_w[...].T
    weights[1] = right_w[...].T
    gain_col[...] = jnp.broadcast_to(mid_gain[...], (128, 128)).T

    def turn(side, v):
        return lax.dot_general(weights[side], v, (((1,), (1,)), ((), ())), preferred_element_type=F32)

    def norm(r, _):
        ao, bc = lax.div(r, 3), lax.rem(r, 3)
        v = x_ref[pl.ds(ao * 8, 8), pl.ds(pl.multiple_of(bc * 16, 16), 16), :].astype(F32).reshape(128, 128)
        v = v - jnp.mean(v, axis=1, keepdims=True)
        v = v * lax.rsqrt(jnp.mean(v * v, axis=1, keepdims=True) + 1e-05) * in_gain[...]
        v = v.astype(BF16)
        ready[r] = v
        wide_r[pl.ds(r, 128, stride=18), :] = turn(1, v)
        return 0

    def project(ao, _):
        for bc in range(3):
            wide_l[bc, pl.ds(ao, 128, stride=6), :] = turn(0, ready[ao * 3 + bc])
        return 0

    def convert(source, target):
        def step(i, _):
            rows = pl.ds(pl.multiple_of(i * 256, 256), 256)
            target[rows, :] = source[rows, :].astype(target.dtype)
            return 0

        lax.fori_loop(0, source.shape[0] // 256, step, 0)

    def start(source, target, send_sem, recv_sem, chunk, slot, device):
        rows = source.shape[0] // 128
        pltpu.make_async_remote_copy(
            src_ref=source.at[pl.ds(chunk * rows, rows)],
            dst_ref=target.at[pl.ds(slot * rows, rows)],
            send_sem=send_sem,
            recv_sem=recv_sem,
            device_id=device,
            device_id_type=MESH,
        ).start()

    def send(*refs):
        def act(column, is_own):
            for o in (7, 3, 4, 0, 2, 5, 1, 6):
                layer, c = (near[o], 0) if o < 4 else (near[(o + 1) % 8], 1)
                args = (column * 8 + near[o], second * 8 + o % 4 * 2 + core, (layer * 2 + c, column))
                if is_own and o in (0, 7):
                    pl.when(core == (1 if o == 0 else 0))(lambda args=args: start(*refs, *args))
                else:
                    start(*refs, *args)

        each_column(act)

    def send_back(*refs):
        def act(column, is_own):
            for p in (0, 6, 2, 5, 1, 7, 3, 4):
                args = (column * 8 + p, second * 8 + a_own, (mine[p // 2] * 2 + p % 2, column))
                if is_own and p in (1, 6):
                    pl.when(core == (1 if p == 6 else 0))(lambda args=args: start(*refs, *args))
                else:
                    start(*refs, *args)

        each_column(act)

    def settle(source, target, sem):
        rows = pl.ds(0, source.shape[0] // 128 * 127)
        pltpu.make_async_copy(source.at[rows], target.at[rows], sem).wait()

    def receive(wide, source, target, spread, sem, chunk, slot):
        settle(source, target, sem)
        convert(target, spread)
        rows = source.shape[0] // 128
        own = wide[pl.ds((second * 8 + chunk) * rows, rows), :]
        spread[pl.ds((second * 8 + slot) * rows, rows), :] = own.astype(BF16).astype(F32)

    lax.fori_loop(0, 18, norm, 0, unroll=3)
    convert(wide_r, sent_r)
    pl.semaphore_wait(barrier, 176)
    send(sent_r, got_r, send_in.at[0], recv_in.at[0])
    lax.fori_loop(0, 6, project, 0)

    def send_left(bc):
        convert(wide_l.at[bc], sent_l.at[bc])
        send(sent_l.at[bc], got_l.at[bc], send_in.at[1 + bc], recv_in.at[1 + bc])

    send_left(0)
    send_left(1)

    def gate(r, _):
        g = jnp.dot(ready[r], gate_w[...], preferred_element_type=F32)
        gates[r] = jax.nn.sigmoid(g)
        return 0

    lax.fori_loop(0, 18, gate, 0, unroll=3)

    def gather_right(t, _):
        bc, h = lax.div(t, 2), lax.rem(t, 2)
        lanes = pl.ds(pl.multiple_of(t * 128, 128), 128)
        for ao in range(6):
            parts = [spread_r[pl.ds((h * 8 + p) * 144 + ao * 3 + bc, 8, stride=18), :] for p in range(8)]
            right[ao * 64 : ao * 64 + 64, lanes] = jnp.concatenate(swap_blocks(parts), axis=0).astype(BF16)
        return 0

    def gather_left(bc, half, layers):
        for pair in range(3):
            pieces = []
            for ao in (2 * pair, 2 * pair + 1):
                pieces += swap_blocks(
                    [
                        spread_l[bc, pl.ds((layers[p // 2] * 2 + p % 2) * 48 + ao, 8, stride=6), :]
                        for p in range(8)
                    ]
                )
            block = jnp.concatenate(pieces, axis=0).astype(BF16)
            left[bc, half * 128 : half * 128 + 128, pair * 128 : pair * 128 + 128] = block.T

    def swap(bc):
        return pltpu.make_async_remote_copy(
            src_ref=outbox.at[bc],
            dst_ref=inbox.at[bc],
            send_sem=send_swap.at[bc],
            recv_sem=recv_swap.at[bc],
            device_id=partner,
            device_id_type=MESH,
        )

    def multiply(bc):
        gather_left(bc, 0, theirs)
        outbox[bc] = jnp.dot(left[bc, 0:128, :], right[...], preferred_element_type=F32).astype(BF16)
        swap(bc).start()
        gather_left(bc, 1, mine)
        part = jnp.dot(left[bc, 128:256, :], right[...], preferred_element_type=F32)
        for zz in range(8):
            for g in range(6):
                sums[g, (bc * 8 + zz) * PITCH : (bc * 8 + zz) * PITCH + 16, :] = part[
                    zz * 16 : zz * 16 + 16, g * 128 : g * 128 + 128
                ]

    def scatter(bc):
        swap(bc).wait_recv()
        for zz in range(8):
            for g in range(6):
                rows = slice((bc * 8 + zz) * PITCH, (bc * 8 + zz) * PITCH + 16)
                there = inbox[bc, zz * 16 : zz * 16 + 16, g * 128 : g * 128 + 128].astype(F32)
                sums[g, rows, :] = (sums[g, rows, :] + there) * 768 ** (-0.5)

        def step(g, _):
            h, bd = lax.rem(g, 2), lax.div(g, 2)
            for ao in range(2):
                parts = [
                    sums[g, pl.ds(bc * 8 * PITCH + ao * 8 + a8, 8, stride=PITCH), :] for a8 in range(8)
                ]
                for p, part in enumerate(swap_blocks(parts)):
                    wide_o[bc, pl.ds((h * 8 + p) * 48 + ao * 3 + bd, 8, stride=6), :] = part
            return 0

        lax.fori_loop(0, 6, step, 0, unroll=3)

    def finish(part):
        def step(r, _):
            v = spread_o[part, pl.ds(r, 128, stride=6), :]
            v = v - jnp.mean(v, axis=0, keepdims=True)
            v = v * lax.rsqrt(jnp.mean(v * v, axis=0, keepdims=True) + 1e-05) * gain_col[...]
            out = jnp.dot(v.astype(BF16).T, out_w[...], preferred_element_type=F32) * gates[part * 6 + r]
            ao, bc = part * 2 + lax.div(r, 3), lax.rem(r, 3)
            o_ref[pl.ds(ao * 8, 8), pl.ds(pl.multiple_of(bc * 16, 16), 16), :] = out.astype(BF16).reshape(8, 16, 128)
            return 0

        lax.fori_loop(0, 6, step, 0, unroll=6)

    def take(bc):
        receive(wide_l.at[bc], sent_l.at[bc], got_l.at[bc], spread_l.at[bc], recv_in.at[1 + bc], a_own, core * 7)
        multiply(bc)

    def give(bc):
        scatter(bc)
        convert(wide_o.at[bc], sent_o.at[bc])
        send_back(sent_o.at[bc], got_o.at[bc], send_out.at[bc], recv_out.at[bc])

    receive(wide_r, sent_r, got_r, spread_r, recv_in.at[0], a_own, core * 7)
    send_left(2)
    lax.fori_loop(0, 6, gather_right, 0, unroll=2)
    for bc in range(3):
        take(bc)
    for bc in range(3):
        give(bc)
    for part in range(3):
        receive(
            wide_o.at[part], sent_o.at[part], got_o.at[part], spread_o.at[part], recv_out.at[part],
            6 - 5 * core, a_own,
        )
        finish(part)

    settle(sent_r, got_r, send_in.at[0])
    for part in range(3):
        settle(sent_l.at[part], got_l.at[part], send_in.at[1 + part])
        settle(sent_o.at[part], got_o.at[part], send_out.at[part])
        swap(part).wait_send()


def shards(pair_rows, in_gain, left_weight, right_weight, mid_gain, out_weight, out_gate):
    hbm = pl.BlockSpec(memory_space=pltpu.HBM)
    square = pltpu.VMEM((128, 128), BF16)
    line = pltpu.VMEM((1, 128), F32)
    def flat(*parts):
        return [pltpu.VMEM(parts + (128,), dtype) for dtype in (F32, BF16, BF16, F32)]

    return pl.pallas_call(
        kernel,
        out_shape=pltpu.VMEM(pair_rows.shape, BF16),
        in_specs=[hbm] * 7,
        out_specs=pl.BlockSpec(memory_space=pltpu.VMEM),
        scratch_shapes=[
            pltpu.VMEM(pair_rows.shape, BF16), line, square, square, line, square, square,
            pltpu.VMEM((2, 128, 128), BF16),
            pltpu.VMEM((18, 128, 128), BF16),
        ]
        + flat(128 * 18)
        + flat(3, 128 * 6)
        + [
            pltpu.VMEM((3, 256, 384), BF16),
            pltpu.VMEM((384, 768), BF16),
            pltpu.VMEM((3, 128, 768), BF16),
            pltpu.VMEM((3, 128, 768), BF16),
            pltpu.VMEM((6, 24 * PITCH, 128), F32),
        ]
        + flat(3, 128 * 6)
        + [
            pltpu.VMEM((18, 128, 128), F32),
            pltpu.VMEM((128, 128), F32),
        ]
        + [pltpu.SemaphoreType.DMA((n,)) for n in (7, 4, 4, 3, 3, 3, 3)],
        compiler_params=pltpu.CompilerParams(
            collective_id=0, has_side_effects=True
        ),
    )(
        pair_rows, in_gain.reshape(1, 128), left_weight, right_weight,
        mid_gain.reshape(1, 128), out_weight, out_gate,
    )


def solution(mesh):
    in_specs = (P("first", "second", None), P(), P(), P(), P(), P(), P())
    out_specs = P("first", "second", None)
    return jax.shard_map(shards, mesh=mesh, in_specs=in_specs, out_specs=out_specs, check_vma=False)
```

```python
import jax
import jax.numpy as jnp
from jax import lax
from jax.experimental import pallas as pl
from jax.experimental.pallas import tpu as pltpu
from jax.sharding import PartitionSpec as P

MESH = pl.DeviceIdType.MESH
F32, BF16 = jnp.float32, jnp.bfloat16
PITCH = 24


def swap_blocks(parts):
    block = lax.broadcasted_iota(jnp.int32, parts[0].shape, 1) // 16
    for h in (4, 2, 1):
        low = (block // h) % 2 == 0
        out = list(parts)
        for p in range(8):
            if p // h % 2 == 0:
                a, b = parts[p], parts[p + h]
                out[p] = jnp.where(low, a, pltpu.roll(b, 16 * h, 1))
                out[p + h] = jnp.where(low, pltpu.roll(a, 128 - 16 * h, 1), b)
        parts = out
    return parts


def kernel(
    x_hbm, in_gain_hbm, left_hbm, right_hbm, mid_gain_hbm, out_hbm, gate_hbm, o_ref,
    x_ref, in_gain, left_w, right_w, mid_gain, out_w, gate_w,
    weights, ready, wide_r, sent_r, got_r, spread_r, wide_l, sent_l, got_l, spread_l,
    left, right, outbox, inbox, sums, wide_o, sent_o, got_o, spread_o, wide_p, sent_p, got_p, spread_p, gates, gain_col,
    load_sem, send_in, recv_in, send_swap, recv_swap, send_out, recv_out,
):
    first, second = lax.axis_index("first"), lax.axis_index("second")
    z, core, y, x = lax.div(first, 2), lax.rem(first, 2), lax.div(second, 4), lax.rem(second, 4)
    a_own = lax.rem(z + 8 - core, 8)
    partner = (lax.rem(z + 1 + 6 * core, 8) * 2 + 1 - core, second)
    mine = [lax.rem(z + 5 - 5 * core + j, 8) for j in range(4)]
    theirs = [lax.rem(z + 1 + 3 * core + j, 8) for j in range(4)]
    near = [lax.rem(z + d, 8) for d in range(8)]

    loads = [
        pltpu.make_async_copy(src, dst, load_sem.at[i])
        for i, (src, dst) in enumerate(
            [
                (x_hbm, x_ref), (right_hbm, right_w), (in_gain_hbm, in_gain), (left_hbm, left_w),
                (mid_gain_hbm, mid_gain), (out_hbm, out_w), (gate_hbm, gate_w),
            ]
        )
    ]
    for load in loads:
        load.start()

    def each_column(act):
        def ahead(i):
            return jnp.where(i == 0, 2, jnp.where(i == 1, 1, jnp.where(i == 2, 3, 0)))

        def step(e, _):
            act(lax.rem(y + ahead(lax.div(e, 4)), 4) * 4 + lax.rem(x + ahead(lax.rem(e, 4)), 4), False)
            return 0

        lax.fori_loop(0, 15, step, 0)
        act(second, True)

    barrier = pltpu.get_barrier_semaphore()

    def greet(column, is_own):
        targets = [(near[d], core) for d in (-3, 3, -2, 2, -1, 1)] + ([] if is_own else [(z, core)])
        for layer, c in targets + [(layer, 1 - core) for layer in mine]:
            pl.semaphore_signal(barrier, inc=1, device_id=(layer * 2 + c, column), device_id_type=MESH)

    each_column(greet)
    pl.semaphore_signal(barrier, inc=1, device_id=partner, device_id_type=MESH)
    for load in loads:
        load.wait()

    weights[0] = left_w[...].T
    weights[1] = right_w[...].T
    gain_col[...] = jnp.broadcast_to(mid_gain[...], (128, 128)).T

    def turn(side, v):
        return lax.dot_general(weights[side], v, (((1,), (1,)), ((), ())), preferred_element_type=F32)

    def norm(r, _):
        ao, bc = lax.div(r, 3), lax.rem(r, 3)
        v = x_ref[pl.ds(ao * 8, 8), pl.ds(pl.multiple_of(bc * 16, 16), 16), :].astype(F32).reshape(128, 128)
        v = v - jnp.mean(v, axis=1, keepdims=True)
        v = v * lax.rsqrt(jnp.mean(v * v, axis=1, keepdims=True) + 1e-05) * in_gain[...]
        v = v.astype(BF16)
        ready[r] = v
        wide_r[pl.ds(r, 128, stride=18), :] = turn(1, v)
        return 0

    def project(ao, _):
        for bc in range(3):
            wide_l[bc, pl.ds(ao, 128, stride=6), :] = turn(0, ready[ao * 3 + bc])
        return 0

    def convert(source, target):
        def step(i, _):
            rows = pl.ds(pl.multiple_of(i * 256, 256), 256)
            target[rows, :] = source[rows, :].astype(target.dtype)
            return 0

        lax.fori_loop(0, source.shape[0] // 256, step, 0)

    def start(source, target, send_sem, recv_sem, chunk, slot, device):
        rows = source.shape[0] // 128
        pltpu.make_async_remote_copy(
            src_ref=source.at[pl.ds(chunk * rows, rows)],
            dst_ref=target.at[pl.ds(slot * rows, rows)],
            send_sem=send_sem,
            recv_sem=recv_sem,
            device_id=device,
            device_id_type=MESH,
        ).start()

    def send(*refs):
        def act(column, is_own):
            for o in (7, 3, 4, 0, 2, 5, 1, 6):
                layer, c = (near[o], 0) if o < 4 else (near[(o + 1) % 8], 1)
                args = (column * 8 + near[o], second * 8 + o % 4 * 2 + core, (layer * 2 + c, column))
                if is_own and o in (0, 7):
                    pl.when(core == (1 if o == 0 else 0))(lambda args=args: start(*refs, *args))
                else:
                    start(*refs, *args)

        each_column(act)

    def send_back(*refs):
        def act(column, is_own):
            for p in (0, 6, 2, 5, 1, 7, 3, 4):
                args = (column * 8 + p, second * 8 + a_own, (mine[p // 2] * 2 + p % 2, column))
                if is_own and p in (1, 6):
                    pl.when(core == (1 if p == 6 else 0))(lambda args=args: start(*refs, *args))
                else:
                    start(*refs, *args)

        each_column(act)

    def settle(source, target, sem):
        rows = pl.ds(0, source.shape[0] // 128 * 127)
        pltpu.make_async_copy(source.at[rows], target.at[rows], sem).wait()

    def receive(wide, source, target, spread, sem, chunk, slot):
        settle(source, target, sem)
        convert(target, spread)
        rows = source.shape[0] // 128
        own = wide[pl.ds((second * 8 + chunk) * rows, rows), :]
        spread[pl.ds((second * 8 + slot) * rows, rows), :] = own.astype(BF16).astype(F32)

    lax.fori_loop(0, 18, norm, 0, unroll=3)
    convert(wide_r, sent_r)
    pl.semaphore_wait(barrier, 176)
    send(sent_r, got_r, send_in.at[0], recv_in.at[0])
    lax.fori_loop(0, 6, project, 0)

    def send_left(bc):
        convert(wide_l.at[bc], sent_l.at[bc])
        send(sent_l.at[bc], got_l.at[bc], send_in.at[1 + bc], recv_in.at[1 + bc])

    send_left(0)
    send_left(1)

    def gate(r, _):
        g = jnp.dot(ready[r], gate_w[...], preferred_element_type=F32)
        gates[r] = jax.nn.sigmoid(g)
        return 0

    lax.fori_loop(0, 18, gate, 0, unroll=3)

    def gather_right(t, _):
        bc, h = lax.div(t, 2), lax.rem(t, 2)
        lanes = pl.ds(pl.multiple_of(t * 128, 128), 128)
        for ao in range(6):
            parts = [spread_r[pl.ds((h * 8 + p) * 144 + ao * 3 + bc, 8, stride=18), :] for p in range(8)]
            right[ao * 64 : ao * 64 + 64, lanes] = jnp.concatenate(swap_blocks(parts), axis=0).astype(BF16)
        return 0

    def gather_left(bc, half, layers):
        for pair in range(3):
            pieces = []
            for ao in (2 * pair, 2 * pair + 1):
                pieces += swap_blocks(
                    [
                        spread_l[bc, pl.ds((layers[p // 2] * 2 + p % 2) * 48 + ao, 8, stride=6), :]
                        for p in range(8)
                    ]
                )
            block = jnp.concatenate(pieces, axis=0).astype(BF16)
            left[bc, half * 128 : half * 128 + 128, pair * 128 : pair * 128 + 128] = block.T

    def swap(bc):
        return pltpu.make_async_remote_copy(
            src_ref=outbox.at[bc],
            dst_ref=inbox.at[bc],
            send_sem=send_swap.at[bc],
            recv_sem=recv_swap.at[bc],
            device_id=partner,
            device_id_type=MESH,
        )

    def multiply(bc):
        gather_left(bc, 0, theirs)
        outbox[bc] = jnp.dot(left[bc, 0:128, :], right[...], preferred_element_type=F32).astype(BF16)
        swap(bc).start()
        gather_left(bc, 1, mine)
        part = jnp.dot(left[bc, 128:256, :], right[...], preferred_element_type=F32)
        for zz in range(8):
            for g in range(6):
                sums[g, (bc * 8 + zz) * PITCH : (bc * 8 + zz) * PITCH + 16, :] = part[
                    zz * 16 : zz * 16 + 16, g * 128 : g * 128 + 128
                ]

    def scatter(bc):
        swap(bc).wait_recv()
        for zz in range(8):
            for g in range(6):
                rows = slice((bc * 8 + zz) * PITCH, (bc * 8 + zz) * PITCH + 16)
                there = inbox[bc, zz * 16 : zz * 16 + 16, g * 128 : g * 128 + 128].astype(F32)
                sums[g, rows, :] = (sums[g, rows, :] + there) * 768 ** (-0.5)

        wide, skip = (wide_o, 0) if bc < 2 else (wide_p, 4)
        count = wide.shape[0] // 128

        def step(g, _):
            h, bd = lax.rem(g, 2), lax.div(g, 2)
            for ao in range(2):
                parts = [
                    sums[g, pl.ds(bc * 8 * PITCH + ao * 8 + a8, 8, stride=PITCH), :] for a8 in range(8)
                ]
                for p, part in enumerate(swap_blocks(parts)):
                    at = (h * 8 + p) * 8 * count + (2 * bc + ao - skip) * 3 + bd
                    wide[pl.ds(at, 8, stride=count), :] = part
            return 0

        lax.fori_loop(0, 6, step, 0, unroll=3)

    def finish(spread, skip):
        count = spread.shape[0] // 128

        def step(r, _):
            v = spread[pl.ds(r, 128, stride=count), :]
            v = v - jnp.mean(v, axis=0, keepdims=True)
            v = v * lax.rsqrt(jnp.mean(v * v, axis=0, keepdims=True) + 1e-05) * gain_col[...]
            out = jnp.dot(v.astype(BF16).T, out_w[...], preferred_element_type=F32) * gates[skip * 3 + r]
            ao, bc = skip + lax.div(r, 3), lax.rem(r, 3)
            o_ref[pl.ds(ao * 8, 8), pl.ds(pl.multiple_of(bc * 16, 16), 16), :] = out.astype(BF16).reshape(8, 16, 128)
            return 0

        lax.fori_loop(0, count, step, 0, unroll=6)

    def take(bc):
        receive(wide_l.at[bc], sent_l.at[bc], got_l.at[bc], spread_l.at[bc], recv_in.at[1 + bc], a_own, core * 7)
        multiply(bc)

    def give(wide, sent, got, i):
        convert(wide, sent)
        send_back(sent, got, send_out.at[i], recv_out.at[i])

    receive(wide_r, sent_r, got_r, spread_r, recv_in.at[0], a_own, core * 7)
    send_left(2)
    lax.fori_loop(0, 6, gather_right, 0, unroll=2)
    for bc in range(3):
        take(bc)
    scatter(0)
    scatter(1)
    give(wide_o, sent_o, got_o, 0)
    scatter(2)
    give(wide_p, sent_p, got_p, 1)
    receive(wide_o, sent_o, got_o, spread_o, recv_out.at[0], 6 - 5 * core, a_own)
    finish(spread_o, 0)
    receive(wide_p, sent_p, got_p, spread_p, recv_out.at[1], 6 - 5 * core, a_own)
    finish(spread_p, 4)

    settle(sent_r, got_r, send_in.at[0])
    settle(sent_o, got_o, send_out.at[0])
    settle(sent_p, got_p, send_out.at[1])
    for part in range(3):
        settle(sent_l.at[part], got_l.at[part], send_in.at[1 + part])
        swap(part).wait_send()


def shards(pair_rows, in_gain, left_weight, right_weight, mid_gain, out_weight, out_gate):
    hbm = pl.BlockSpec(memory_space=pltpu.HBM)
    square = pltpu.VMEM((128, 128), BF16)
    line = pltpu.VMEM((1, 128), F32)
    def flat(*parts):
        return [pltpu.VMEM(parts + (128,), dtype) for dtype in (F32, BF16, BF16, F32)]

    return pl.pallas_call(
        kernel,
        out_shape=pltpu.VMEM(pair_rows.shape, BF16),
        in_specs=[hbm] * 7,
        out_specs=pl.BlockSpec(memory_space=pltpu.VMEM),
        scratch_shapes=[
            pltpu.VMEM(pair_rows.shape, BF16), line, square, square, line, square, square,
            pltpu.VMEM((2, 128, 128), BF16),
            pltpu.VMEM((18, 128, 128), BF16),
        ]
        + flat(128 * 18)
        + flat(3, 128 * 6)
        + [
            pltpu.VMEM((3, 256, 384), BF16),
            pltpu.VMEM((384, 768), BF16),
            pltpu.VMEM((3, 128, 768), BF16),
            pltpu.VMEM((3, 128, 768), BF16),
            pltpu.VMEM((6, 24 * PITCH, 128), F32),
        ]
        + flat(128 * 12)
        + flat(128 * 6)
        + [
            pltpu.VMEM((18, 128, 128), F32),
            pltpu.VMEM((128, 128), F32),
        ]
        + [pltpu.SemaphoreType.DMA((n,)) for n in (7, 4, 4, 3, 3, 2, 2)],
        compiler_params=pltpu.CompilerParams(
            collective_id=0, has_side_effects=True
        ),
    )(
        pair_rows, in_gain.reshape(1, 128), left_weight, right_weight,
        mid_gain.reshape(1, 128), out_weight, out_gate,
    )


def solution(mesh):
    in_specs = (P("first", "second", None), P(), P(), P(), P(), P(), P())
    out_specs = P("first", "second", None)
    return jax.shard_map(shards, mesh=mesh, in_specs=in_specs, out_specs=out_specs, check_vma=False)
```

```python
import jax
import jax.numpy as jnp
from jax import lax
from jax.experimental import pallas as pl
from jax.experimental.pallas import tpu as pltpu
from jax.sharding import PartitionSpec as P

MESH = pl.DeviceIdType.MESH
F32, BF16 = jnp.float32, jnp.bfloat16
PITCH = 24


def swap_blocks(parts):
    block = lax.broadcasted_iota(jnp.int32, parts[0].shape, 1) // 16
    for h in (4, 2, 1):
        low = (block // h) % 2 == 0
        out = list(parts)
        for p in range(8):
            if p // h % 2 == 0:
                a, b = parts[p], parts[p + h]
                out[p] = jnp.where(low, a, pltpu.roll(b, 16 * h, 1))
                out[p + h] = jnp.where(low, pltpu.roll(a, 128 - 16 * h, 1), b)
        parts = out
    return parts


def kernel(
    x_hbm, in_gain_hbm, left_hbm, right_hbm, mid_gain_hbm, out_hbm, gate_hbm, o_ref,
    x_ref, in_gain, left_w, right_w, mid_gain, out_w, gate_w,
    weights, ready, wide_r, sent_r, got_r, spread_r, wide_l, sent_l, got_l, spread_l,
    left, right, outbox, inbox, sums, wide_o, sent_o, got_o, spread_o, wide_p, sent_p, got_p, spread_p, gates, gain_col,
    load_sem, send_in, recv_in, send_swap, recv_swap, send_out, recv_out,
):
    first, second = lax.axis_index("first"), lax.axis_index("second")
    z, core, y, x = lax.div(first, 2), lax.rem(first, 2), lax.div(second, 4), lax.rem(second, 4)
    a_own = lax.rem(z + 8 - core, 8)
    partner = (lax.rem(z + 1 + 6 * core, 8) * 2 + 1 - core, second)
    mine = [lax.rem(z + 5 - 5 * core + j, 8) for j in range(4)]
    theirs = [lax.rem(z + 1 + 3 * core + j, 8) for j in range(4)]
    near = [lax.rem(z + d, 8) for d in range(8)]

    loads = [
        pltpu.make_async_copy(src, dst, load_sem.at[i])
        for i, (src, dst) in enumerate(
            [
                (x_hbm, x_ref), (right_hbm, right_w), (in_gain_hbm, in_gain), (left_hbm, left_w),
                (mid_gain_hbm, mid_gain), (out_hbm, out_w), (gate_hbm, gate_w),
            ]
        )
    ]
    for load in loads:
        load.start()

    def each_column(act):
        def ahead(i):
            return jnp.where(i == 0, 2, jnp.where(i == 1, 1, jnp.where(i == 2, 3, 0)))

        def step(e, _):
            act(lax.rem(y + ahead(lax.div(e, 4)), 4) * 4 + lax.rem(x + ahead(lax.rem(e, 4)), 4), False)
            return 0

        lax.fori_loop(0, 15, step, 0)
        act(second, True)

    barrier = pltpu.get_barrier_semaphore()

    def greet(column, is_own):
        targets = [(near[d], core) for d in (-3, 3, -2, 2, -1, 1)] + ([] if is_own else [(z, core)])
        for layer, c in targets + [(layer, 1 - core) for layer in mine]:
            pl.semaphore_signal(barrier, inc=1, device_id=(layer * 2 + c, column), device_id_type=MESH)

    each_column(greet)
    pl.semaphore_signal(barrier, inc=1, device_id=partner, device_id_type=MESH)
    for load in loads:
        load.wait()

    weights[0] = left_w[...].T
    weights[1] = right_w[...].T
    gain_col[...] = jnp.broadcast_to(mid_gain[...], (128, 128)).T

    def turn(side, v):
        return lax.dot_general(weights[side], v, (((1,), (1,)), ((), ())), preferred_element_type=F32)

    def norm(r, _):
        ao, bc = lax.div(r, 3), lax.rem(r, 3)
        v = x_ref[pl.ds(ao * 8, 8), pl.ds(pl.multiple_of(bc * 16, 16), 16), :].astype(F32).reshape(128, 128)
        v = v - jnp.mean(v, axis=1, keepdims=True)
        v = v * lax.rsqrt(jnp.mean(v * v, axis=1, keepdims=True) + 1e-05) * in_gain[...]
        v = v.astype(BF16)
        ready[r] = v
        wide_r[pl.ds(r, 128, stride=18), :] = turn(1, v)
        return 0

    def project(ao, _):
        for bc in range(3):
            wide_l[bc, pl.ds(ao, 128, stride=6), :] = turn(0, ready[ao * 3 + bc])
        return 0

    def convert(source, target):
        def step(i, _):
            rows = pl.ds(pl.multiple_of(i * 256, 256), 256)
            target[rows, :] = source[rows, :].astype(target.dtype)
            return 0

        lax.fori_loop(0, source.shape[0] // 256, step, 0)

    def start(source, target, send_sem, recv_sem, chunk, slot, device):
        rows = source.shape[0] // 128
        pltpu.make_async_remote_copy(
            src_ref=source.at[pl.ds(chunk * rows, rows)],
            dst_ref=target.at[pl.ds(slot * rows, rows)],
            send_sem=send_sem,
            recv_sem=recv_sem,
            device_id=device,
            device_id_type=MESH,
        ).start()

    def send(*refs):
        def act(column, is_own):
            for o in (7, 3, 4, 0, 2, 5, 1, 6):
                layer, c = (near[o], 0) if o < 4 else (near[(o + 1) % 8], 1)
                args = (column * 8 + near[o], second * 8 + o % 4 * 2 + core, (layer * 2 + c, column))
                if is_own and o in (0, 7):
                    pl.when(core == (1 if o == 0 else 0))(lambda args=args: start(*refs, *args))
                else:
                    start(*refs, *args)

        each_column(act)

    def send_back(*refs):
        def act(column, is_own):
            for p in (0, 6, 2, 5, 1, 7, 3, 4):
                args = (column * 8 + p, second * 8 + a_own, (mine[p // 2] * 2 + p % 2, column))
                if is_own and p in (1, 6):
                    pl.when(core == (1 if p == 6 else 0))(lambda args=args: start(*refs, *args))
                else:
                    start(*refs, *args)

        each_column(act)

    def settle(source, target, sem):
        rows = pl.ds(0, source.shape[0] // 128 * 127)
        pltpu.make_async_copy(source.at[rows], target.at[rows], sem).wait()

    def receive(wide, source, target, spread, sem, chunk, slot):
        settle(source, target, sem)
        convert(target, spread)
        rows = source.shape[0] // 128
        own = wide[pl.ds((second * 8 + chunk) * rows, rows), :]
        spread[pl.ds((second * 8 + slot) * rows, rows), :] = own.astype(BF16).astype(F32)

    lax.fori_loop(0, 18, norm, 0, unroll=3)
    convert(wide_r, sent_r)
    pl.semaphore_wait(barrier, 176)
    send(sent_r, got_r, send_in.at[0], recv_in.at[0])
    lax.fori_loop(0, 6, project, 0)

    def send_left(bc):
        convert(wide_l.at[bc], sent_l.at[bc])
        send(sent_l.at[bc], got_l.at[bc], send_in.at[1 + bc], recv_in.at[1 + bc])

    send_left(0)
    send_left(1)

    def gate(r, _):
        g = jnp.dot(ready[r], gate_w[...], preferred_element_type=F32)
        gates[r] = jax.nn.sigmoid(g)
        return 0

    lax.fori_loop(0, 18, gate, 0, unroll=3)

    def gather_right(t, _):
        bc, h = lax.div(t, 2), lax.rem(t, 2)
        lanes = pl.ds(pl.multiple_of(t * 128, 128), 128)
        for ao in range(6):
            parts = [spread_r[pl.ds((h * 8 + p) * 144 + ao * 3 + bc, 8, stride=18), :] for p in range(8)]
            right[ao * 64 : ao * 64 + 64, lanes] = jnp.concatenate(swap_blocks(parts), axis=0).astype(BF16)
        return 0

    def gather_left(bc, half, layers):
        for pair in range(3):
            pieces = []
            for ao in (2 * pair, 2 * pair + 1):
                pieces += swap_blocks(
                    [
                        spread_l[bc, pl.ds((layers[p // 2] * 2 + p % 2) * 48 + ao, 8, stride=6), :]
                        for p in range(8)
                    ]
                )
            block = jnp.concatenate(pieces, axis=0).astype(BF16)
            left[bc, half * 128 : half * 128 + 128, pair * 128 : pair * 128 + 128] = block.T

    def swap(bc):
        return pltpu.make_async_remote_copy(
            src_ref=outbox.at[bc],
            dst_ref=inbox.at[bc],
            send_sem=send_swap.at[bc],
            recv_sem=recv_swap.at[bc],
            device_id=partner,
            device_id_type=MESH,
        )

    def multiply_theirs(bc):
        gather_left(bc, 0, theirs)
        outbox[bc] = jnp.dot(left[bc, 0:128, :], right[...], preferred_element_type=F32).astype(BF16)
        swap(bc).start()

    def multiply_mine(bc):
        gather_left(bc, 1, mine)
        part = jnp.dot(left[bc, 128:256, :], right[...], preferred_element_type=F32)
        for zz in range(8):
            for g in range(6):
                sums[g, (bc * 8 + zz) * PITCH : (bc * 8 + zz) * PITCH + 16, :] = part[
                    zz * 16 : zz * 16 + 16, g * 128 : g * 128 + 128
                ]

    def scatter(bc):
        swap(bc).wait_recv()
        for zz in range(8):
            for g in range(6):
                rows = slice((bc * 8 + zz) * PITCH, (bc * 8 + zz) * PITCH + 16)
                there = inbox[bc, zz * 16 : zz * 16 + 16, g * 128 : g * 128 + 128].astype(F32)
                sums[g, rows, :] = (sums[g, rows, :] + there) * 768 ** (-0.5)

        wide, skip = (wide_o, 0) if bc < 2 else (wide_p, 4)
        count = wide.shape[0] // 128

        def step(g, _):
            h, bd = lax.rem(g, 2), lax.div(g, 2)
            for ao in range(2):
                parts = [
                    sums[g, pl.ds(bc * 8 * PITCH + ao * 8 + a8, 8, stride=PITCH), :] for a8 in range(8)
                ]
                for p, part in enumerate(swap_blocks(parts)):
                    at = (h * 8 + p) * 8 * count + (2 * bc + ao - skip) * 3 + bd
                    wide[pl.ds(at, 8, stride=count), :] = part
            return 0

        lax.fori_loop(0, 6, step, 0, unroll=3)

    def finish(spread, skip):
        count = spread.shape[0] // 128

        def step(r, _):
            v = spread[pl.ds(r, 128, stride=count), :]
            v = v - jnp.mean(v, axis=0, keepdims=True)
            v = v * lax.rsqrt(jnp.mean(v * v, axis=0, keepdims=True) + 1e-05) * gain_col[...]
            out = jnp.dot(v.astype(BF16).T, out_w[...], preferred_element_type=F32) * gates[skip * 3 + r]
            ao, bc = skip + lax.div(r, 3), lax.rem(r, 3)
            o_ref[pl.ds(ao * 8, 8), pl.ds(pl.multiple_of(bc * 16, 16), 16), :] = out.astype(BF16).reshape(8, 16, 128)
            return 0

        lax.fori_loop(0, count, step, 0, unroll=6)

    def take(bc):
        receive(wide_l.at[bc], sent_l.at[bc], got_l.at[bc], spread_l.at[bc], recv_in.at[1 + bc], a_own, core * 7)
        multiply_theirs(bc)

    def give(wide, sent, got, i):
        convert(wide, sent)
        send_back(sent, got, send_out.at[i], recv_out.at[i])

    receive(wide_r, sent_r, got_r, spread_r, recv_in.at[0], a_own, core * 7)
    send_left(2)
    lax.fori_loop(0, 6, gather_right, 0, unroll=2)
    for bc in range(3):
        take(bc)
        if bc < 2:
            multiply_mine(bc)
    scatter(0)
    scatter(1)
    give(wide_o, sent_o, got_o, 0)
    multiply_mine(2)
    scatter(2)
    give(wide_p, sent_p, got_p, 1)
    receive(wide_o, sent_o, got_o, spread_o, recv_out.at[0], 6 - 5 * core, a_own)
    finish(spread_o, 0)
    receive(wide_p, sent_p, got_p, spread_p, recv_out.at[1], 6 - 5 * core, a_own)
    finish(spread_p, 4)

    settle(sent_r, got_r, send_in.at[0])
    settle(sent_o, got_o, send_out.at[0])
    settle(sent_p, got_p, send_out.at[1])
    for part in range(3):
        settle(sent_l.at[part], got_l.at[part], send_in.at[1 + part])
        swap(part).wait_send()


def shards(pair_rows, in_gain, left_weight, right_weight, mid_gain, out_weight, out_gate):
    hbm = pl.BlockSpec(memory_space=pltpu.HBM)
    square = pltpu.VMEM((128, 128), BF16)
    line = pltpu.VMEM((1, 128), F32)
    def flat(*parts):
        return [pltpu.VMEM(parts + (128,), dtype) for dtype in (F32, BF16, BF16, F32)]

    return pl.pallas_call(
        kernel,
        out_shape=pltpu.VMEM(pair_rows.shape, BF16),
        in_specs=[hbm] * 7,
        out_specs=pl.BlockSpec(memory_space=pltpu.VMEM),
        scratch_shapes=[
            pltpu.VMEM(pair_rows.shape, BF16), line, square, square, line, square, square,
            pltpu.VMEM((2, 128, 128), BF16),
            pltpu.VMEM((18, 128, 128), BF16),
        ]
        + flat(128 * 18)
        + flat(3, 128 * 6)
        + [
            pltpu.VMEM((3, 256, 384), BF16),
            pltpu.VMEM((384, 768), BF16),
            pltpu.VMEM((3, 128, 768), BF16),
            pltpu.VMEM((3, 128, 768), BF16),
            pltpu.VMEM((6, 24 * PITCH, 128), F32),
        ]
        + flat(128 * 12)
        + flat(128 * 6)
        + [
            pltpu.VMEM((18, 128, 128), F32),
            pltpu.VMEM((128, 128), F32),
        ]
        + [pltpu.SemaphoreType.DMA((n,)) for n in (7, 4, 4, 3, 3, 2, 2)],
        compiler_params=pltpu.CompilerParams(
            collective_id=0, has_side_effects=True
        ),
    )(
        pair_rows, in_gain.reshape(1, 128), left_weight, right_weight,
        mid_gain.reshape(1, 128), out_weight, out_gate,
    )


def solution(mesh):
    in_specs = (P("first", "second", None), P(), P(), P(), P(), P(), P())
    out_specs = P("first", "second", None)
    return jax.shard_map(shards, mesh=mesh, in_specs=in_specs, out_specs=out_specs, check_vma=False)
```

```python
import jax
import jax.numpy as jnp
from jax import lax
from jax.experimental import pallas as pl
from jax.experimental.pallas import tpu as pltpu
from jax.sharding import PartitionSpec as P

MESH = pl.DeviceIdType.MESH
F32, BF16 = jnp.float32, jnp.bfloat16
PITCH = 24


def swap_blocks(parts):
    block = lax.broadcasted_iota(jnp.int32, parts[0].shape, 1) // 16
    for h in (4, 2, 1):
        low = (block // h) % 2 == 0
        out = list(parts)
        for p in range(8):
            if p // h % 2 == 0:
                a, b = parts[p], parts[p + h]
                out[p] = jnp.where(low, a, pltpu.roll(b, 16 * h, 1))
                out[p + h] = jnp.where(low, pltpu.roll(a, 128 - 16 * h, 1), b)
        parts = out
    return parts


def kernel(
    x_hbm, in_gain_hbm, left_hbm, right_hbm, mid_gain_hbm, out_hbm, gate_hbm, o_ref,
    x_ref, in_gain, left_w, right_w, mid_gain, out_w, gate_w,
    weights, ready, wide_r, sent_r, got_r, spread_r, wide_l, sent_l, got_l, spread_l,
    left, right, outbox, inbox, sums, wide_o, sent_o, got_o, spread_o, wide_p, sent_p, got_p, spread_p, gates, gain_col,
    load_sem, send_in, recv_in, send_swap, recv_swap, send_out, recv_out,
):
    first, second = lax.axis_index("first"), lax.axis_index("second")
    z, core, y, x = lax.div(first, 2), lax.rem(first, 2), lax.div(second, 4), lax.rem(second, 4)
    a_own = lax.rem(z + 8 - core, 8)
    partner = (lax.rem(z + 1 + 6 * core, 8) * 2 + 1 - core, second)
    mine = [lax.rem(z + 5 - 5 * core + j, 8) for j in range(4)]
    theirs = [lax.rem(z + 1 + 3 * core + j, 8) for j in range(4)]
    near = [lax.rem(z + d, 8) for d in range(8)]

    loads = [
        pltpu.make_async_copy(src, dst, load_sem.at[i])
        for i, (src, dst) in enumerate(
            [
                (x_hbm, x_ref), (right_hbm, right_w), (in_gain_hbm, in_gain), (left_hbm, left_w),
                (mid_gain_hbm, mid_gain), (out_hbm, out_w), (gate_hbm, gate_w),
            ]
        )
    ]
    for load in loads:
        load.start()

    def each_column(act):
        def ahead(i):
            return jnp.where(i == 0, 2, jnp.where(i == 1, 1, jnp.where(i == 2, 3, 0)))

        def step(e, _):
            act(lax.rem(y + ahead(lax.div(e, 4)), 4) * 4 + lax.rem(x + ahead(lax.rem(e, 4)), 4), False)
            return 0

        lax.fori_loop(0, 15, step, 0)
        act(second, True)

    barrier = pltpu.get_barrier_semaphore()

    def greet(column, is_own):
        targets = [(near[d], core) for d in (-3, 3, -2, 2, -1, 1)] + ([] if is_own else [(z, core)])
        for layer, c in targets + [(layer, 1 - core) for layer in mine]:
            pl.semaphore_signal(barrier, inc=1, device_id=(layer * 2 + c, column), device_id_type=MESH)

    each_column(greet)
    pl.semaphore_signal(barrier, inc=1, device_id=partner, device_id_type=MESH)
    for load in loads:
        load.wait()

    weights[0] = left_w[...].T
    weights[1] = right_w[...].T
    gain_col[...] = jnp.broadcast_to(mid_gain[...], (128, 128)).T

    def turn(side, v):
        return lax.dot_general(weights[side], v, (((1,), (1,)), ((), ())), preferred_element_type=F32)

    def norm(r, _):
        ao, bc = lax.div(r, 3), lax.rem(r, 3)
        v = x_ref[pl.ds(ao * 8, 8), pl.ds(pl.multiple_of(bc * 16, 16), 16), :].astype(F32).reshape(128, 128)
        v = v - jnp.mean(v, axis=1, keepdims=True)
        v = v * lax.rsqrt(jnp.mean(v * v, axis=1, keepdims=True) + 1e-05) * in_gain[...]
        v = v.astype(BF16)
        ready[r] = v
        wide_r[pl.ds(r, 128, stride=18), :] = turn(1, v)
        return 0

    def project(ao, _):
        for bc in range(3):
            wide_l[bc, pl.ds(ao, 128, stride=6), :] = turn(0, ready[ao * 3 + bc])
        return 0

    def convert(source, target):
        def step(i, _):
            rows = pl.ds(pl.multiple_of(i * 256, 256), 256)
            target[rows, :] = source[rows, :].astype(target.dtype)
            return 0

        lax.fori_loop(0, source.shape[0] // 256, step, 0)

    def start(source, target, send_sem, recv_sem, chunk, slot, device):
        rows = source.shape[0] // 128
        pltpu.make_async_remote_copy(
            src_ref=source.at[pl.ds(chunk * rows, rows)],
            dst_ref=target.at[pl.ds(slot * rows, rows)],
            send_sem=send_sem,
            recv_sem=recv_sem,
            device_id=device,
            device_id_type=MESH,
        ).start()

    def send(*refs):
        def act(column, is_own):
            for o in (7, 3, 4, 0, 2, 5, 1, 6):
                layer, c = (near[o], 0) if o < 4 else (near[(o + 1) % 8], 1)
                args = (column * 8 + near[o], second * 8 + o % 4 * 2 + core, (layer * 2 + c, column))
                if is_own and o in (0, 7):
                    pl.when(core == (1 if o == 0 else 0))(lambda args=args: start(*refs, *args))
                else:
                    start(*refs, *args)

        each_column(act)

    def send_back(*refs):
        def act(column, is_own):
            for p in (0, 6, 2, 5, 1, 7, 3, 4):
                args = (column * 8 + p, second * 8 + a_own, (mine[p // 2] * 2 + p % 2, column))
                if is_own and p in (1, 6):
                    pl.when(core == (1 if p == 6 else 0))(lambda args=args: start(*refs, *args))
                else:
                    start(*refs, *args)

        each_column(act)

    def settle(source, target, sem):
        rows = pl.ds(0, source.shape[0] // 128 * 127)
        pltpu.make_async_copy(source.at[rows], target.at[rows], sem).wait()

    def receive(wide, source, target, spread, sem, chunk, slot):
        settle(source, target, sem)
        convert(target, spread)
        rows = source.shape[0] // 128
        own = wide[pl.ds((second * 8 + chunk) * rows, rows), :]
        spread[pl.ds((second * 8 + slot) * rows, rows), :] = own.astype(BF16).astype(F32)

    lax.fori_loop(0, 18, norm, 0, unroll=3)
    convert(wide_r, sent_r)
    lax.fori_loop(0, 6, project, 0)
    pl.semaphore_wait(barrier, 176)
    send(sent_r, got_r, send_in.at[0], recv_in.at[0])

    def send_left(bc):
        convert(wide_l.at[bc], sent_l.at[bc])
        send(sent_l.at[bc], got_l.at[bc], send_in.at[1 + bc], recv_in.at[1 + bc])

    send_left(0)
    send_left(1)

    def gate(r, _):
        g = jnp.dot(ready[r], gate_w[...], preferred_element_type=F32)
        gates[r] = jax.nn.sigmoid(g)
        return 0

    lax.fori_loop(0, 18, gate, 0, unroll=3)

    def gather_right(t, _):
        bc, h = lax.div(t, 2), lax.rem(t, 2)
        lanes = pl.ds(pl.multiple_of(t * 128, 128), 128)
        for ao in range(6):
            parts = [spread_r[pl.ds((h * 8 + p) * 144 + ao * 3 + bc, 8, stride=18), :] for p in range(8)]
            right[ao * 64 : ao * 64 + 64, lanes] = jnp.concatenate(swap_blocks(parts), axis=0).astype(BF16)
        return 0

    def gather_left(bc, half, layers):
        for pair in range(3):
            pieces = []
            for ao in (2 * pair, 2 * pair + 1):
                pieces += swap_blocks(
                    [
                        spread_l[bc, pl.ds((layers[p // 2] * 2 + p % 2) * 48 + ao, 8, stride=6), :]
                        for p in range(8)
                    ]
                )
            block = jnp.concatenate(pieces, axis=0).astype(BF16)
            left[bc, half * 128 : half * 128 + 128, pair * 128 : pair * 128 + 128] = block.T

    def swap(bc):
        return pltpu.make_async_remote_copy(
            src_ref=outbox.at[bc],
            dst_ref=inbox.at[bc],
            send_sem=send_swap.at[bc],
            recv_sem=recv_swap.at[bc],
            device_id=partner,
            device_id_type=MESH,
        )

    def multiply(bc):
        gather_left(bc, 0, theirs)
        outbox[bc] = jnp.dot(left[bc, 0:128, :], right[...], preferred_element_type=F32).astype(BF16)
        swap(bc).start()
        gather_left(bc, 1, mine)
        part = jnp.dot(left[bc, 128:256, :], right[...], preferred_element_type=F32)
        for zz in range(8):
            for g in range(6):
                sums[g, (bc * 8 + zz) * PITCH : (bc * 8 + zz) * PITCH + 16, :] = part[
                    zz * 16 : zz * 16 + 16, g * 128 : g * 128 + 128
                ]

    def scatter(bc):
        swap(bc).wait_recv()
        for zz in range(8):
            for g in range(6):
                rows = slice((bc * 8 + zz) * PITCH, (bc * 8 + zz) * PITCH + 16)
                there = inbox[bc, zz * 16 : zz * 16 + 16, g * 128 : g * 128 + 128].astype(F32)
                sums[g, rows, :] = (sums[g, rows, :] + there) * 768 ** (-0.5)

        wide, skip = (wide_o, 0) if bc < 2 else (wide_p, 4)
        count = wide.shape[0] // 128

        def step(g, _):
            h, bd = lax.rem(g, 2), lax.div(g, 2)
            for ao in range(2):
                parts = [
                    sums[g, pl.ds(bc * 8 * PITCH + ao * 8 + a8, 8, stride=PITCH), :] for a8 in range(8)
                ]
                for p, part in enumerate(swap_blocks(parts)):
                    at = (h * 8 + p) * 8 * count + (2 * bc + ao - skip) * 3 + bd
                    wide[pl.ds(at, 8, stride=count), :] = part
            return 0

        lax.fori_loop(0, 6, step, 0, unroll=3)

    def finish(spread, skip):
        count = spread.shape[0] // 128

        def step(r, _):
            v = spread[pl.ds(r, 128, stride=count), :]
            v = v - jnp.mean(v, axis=0, keepdims=True)
            v = v * lax.rsqrt(jnp.mean(v * v, axis=0, keepdims=True) + 1e-05) * gain_col[...]
            out = jnp.dot(v.astype(BF16).T, out_w[...], preferred_element_type=F32) * gates[skip * 3 + r]
            ao, bc = skip + lax.div(r, 3), lax.rem(r, 3)
            o_ref[pl.ds(ao * 8, 8), pl.ds(pl.multiple_of(bc * 16, 16), 16), :] = out.astype(BF16).reshape(8, 16, 128)
            return 0

        lax.fori_loop(0, count, step, 0, unroll=6)

    def take(bc):
        receive(wide_l.at[bc], sent_l.at[bc], got_l.at[bc], spread_l.at[bc], recv_in.at[1 + bc], a_own, core * 7)
        multiply(bc)

    def give(wide, sent, got, i):
        convert(wide, sent)
        send_back(sent, got, send_out.at[i], recv_out.at[i])

    receive(wide_r, sent_r, got_r, spread_r, recv_in.at[0], a_own, core * 7)
    send_left(2)
    lax.fori_loop(0, 6, gather_right, 0, unroll=2)
    for bc in range(3):
        take(bc)
    scatter(0)
    scatter(1)
    give(wide_o, sent_o, got_o, 0)
    scatter(2)
    give(wide_p, sent_p, got_p, 1)
    receive(wide_o, sent_o, got_o, spread_o, recv_out.at[0], 6 - 5 * core, a_own)
    finish(spread_o, 0)
    receive(wide_p, sent_p, got_p, spread_p, recv_out.at[1], 6 - 5 * core, a_own)
    finish(spread_p, 4)

    settle(sent_r, got_r, send_in.at[0])
    settle(sent_o, got_o, send_out.at[0])
    settle(sent_p, got_p, send_out.at[1])
    for part in range(3):
        settle(sent_l.at[part], got_l.at[part], send_in.at[1 + part])
        swap(part).wait_send()


def shards(pair_rows, in_gain, left_weight, right_weight, mid_gain, out_weight, out_gate):
    hbm = pl.BlockSpec(memory_space=pltpu.HBM)
    square = pltpu.VMEM((128, 128), BF16)
    line = pltpu.VMEM((1, 128), F32)
    def flat(*parts):
        return [pltpu.VMEM(parts + (128,), dtype) for dtype in (F32, BF16, BF16, F32)]

    return pl.pallas_call(
        kernel,
        out_shape=pltpu.VMEM(pair_rows.shape, BF16),
        in_specs=[hbm] * 7,
        out_specs=pl.BlockSpec(memory_space=pltpu.VMEM),
        scratch_shapes=[
            pltpu.VMEM(pair_rows.shape, BF16), line, square, square, line, square, square,
            pltpu.VMEM((2, 128, 128), BF16),
            pltpu.VMEM((18, 128, 128), BF16),
        ]
        + flat(128 * 18)
        + flat(3, 128 * 6)
        + [
            pltpu.VMEM((3, 256, 384), BF16),
            pltpu.VMEM((384, 768), BF16),
            pltpu.VMEM((3, 128, 768), BF16),
            pltpu.VMEM((3, 128, 768), BF16),
            pltpu.VMEM((6, 24 * PITCH, 128), F32),
        ]
        + flat(128 * 12)
        + flat(128 * 6)
        + [
            pltpu.VMEM((18, 128, 128), F32),
            pltpu.VMEM((128, 128), F32),
        ]
        + [pltpu.SemaphoreType.DMA((n,)) for n in (7, 4, 4, 3, 3, 2, 2)],
        compiler_params=pltpu.CompilerParams(
            collective_id=0, has_side_effects=True
        ),
    )(
        pair_rows, in_gain.reshape(1, 128), left_weight, right_weight,
        mid_gain.reshape(1, 128), out_weight, out_gate,
    )


def solution(mesh):
    in_specs = (P("first", "second", None), P(), P(), P(), P(), P(), P())
    out_specs = P("first", "second", None)
    return jax.shard_map(shards, mesh=mesh, in_specs=in_specs, out_specs=out_specs, check_vma=False)
```
